8 devices in a mesh: ep: 8 (over z, y, x, core).
Axes of the slice: x: 2, y: 2, z: 1, core: 2. Of those that a mesh axis runs over, the one named last changes fastest.
Arguments:
- tokens: bfloat16 [1024, 4096], P('ep')
- k_cache: bfloat16 [1024, 64, 32, 128], P('ep')
- v_cache: bfloat16 [1024, 64, 32, 128], P('ep')
- positions: int32 [1024], P('ep')
- expert_one: int32 [1024], P('ep')
- expert_two: int32 [1024], P('ep')
- eligible: int32 [1024, 8], P('ep')
- ln1_gain: bfloat16 [4096], replicated
- ln1_bias: bfloat16 [4096], replicated
- w_query: bfloat16 [4096, 4096], replicated
- b_query: bfloat16 [4096], replicated
- w_key: bfloat16 [4096, 4096], replicated
- b_key: bfloat16 [4096], replicated
- w_value: bfloat16 [4096, 4096], replicated
- b_value: bfloat16 [4096], replicated
- w_out: bfloat16 [4096, 4096], replicated
- b_out: bfloat16 [4096], replicated
- ln2_gain: bfloat16 [4096], replicated
- ln2_bias: bfloat16 [4096], replicated
- w_router: bfloat16 [4096, 8], replicated
- w_gate: bfloat16 [8, 4096, 1376], P('ep')
- w_up: bfloat16 [8, 4096, 1376], P('ep')
- w_down: bfloat16 [8, 1376, 4096], P('ep')
Outputs:
- output 1: bfloat16 [1024, 4096], P('ep')
- output 2: bfloat16 [1024, 32, 128], P('ep')
- output 3: bfloat16 [1024, 32, 128], P('ep')
All inputs are finite; a program needn't handle non-finite values.
Results may differ from the reference program's by a relative error of at most 0.0102763.
Values are sent between devices in bfloat16 or wider.
A program may use at most 1.25 GiB of HBM per device.

```python
import jax
import jax.numpy as jnp
from jax import lax

D_MODEL = 4096
NUM_HEADS = 32
NUM_KV_HEADS = 32
HEAD_DIM = 128
FF_DIM = 1376
NUM_EXPERTS = 8
TOK_DEV = 128
SEQ_LEN = 64
NUM_GROUPS = 8
BATCH = TOK_DEV * NUM_GROUPS
GROUP_SIZE = NUM_HEADS // NUM_KV_HEADS
Q_DIM = NUM_HEADS * HEAD_DIM
KV_DIM = NUM_KV_HEADS * HEAD_DIM
ROPE_BASE = 10000.0
LN_EPS = 1e-5


def draw_normal(key, arr_shape, std_dev):
    return (jax.random.normal(key, arr_shape, jnp.float32) * std_dev).astype(jnp.bfloat16)


def draw_positions(key):
    k_pos, k_top, k_low = jax.random.split(key, 3)
    row_ids = jnp.arange(BATCH)
    pos_vals = jax.random.randint(k_pos, (BATCH,), 0, SEQ_LEN)
    top_row = jax.random.randint(k_top, (), 0, BATCH)
    low_row = (top_row + 1 + jax.random.randint(k_low, (), 0, BATCH - 1)) % BATCH
    pos_vals = jnp.where(row_ids == top_row, SEQ_LEN - 1, pos_vals)
    return jnp.where(row_ids == low_row, 0, pos_vals).astype(jnp.int32)


def draw_routes(key):
    k_mix, k_hot, k_src, k_rot, k_sec, k_elig = jax.random.split(key, 6)
    row_ids = jnp.arange(BATCH)
    mix_draw = jax.random.randint(k_mix, (BATCH,), 0, 4 * NUM_EXPERTS)
    hot_expert = jax.random.randint(k_hot, (), 0, NUM_EXPERTS)
    first_choice = jnp.where(mix_draw < 2 * NUM_EXPERTS, mix_draw % NUM_EXPERTS, (hot_expert + mix_draw % 2) % NUM_EXPERTS)
    src_group = jax.random.randint(k_src, (), 0, NUM_GROUPS)
    first_choice = jnp.where(row_ids // TOK_DEV == src_group, hot_expert, first_choice)
    rotation = jax.random.randint(k_rot, (), 0, NUM_EXPERTS)
    offset_rows = (row_ids - (src_group + 1) * TOK_DEV) % BATCH
    first_choice = jnp.where(offset_rows < NUM_EXPERTS, (offset_rows + rotation) % NUM_EXPERTS, first_choice)
    second_choice = (first_choice + 1 + jax.random.randint(k_sec, (BATCH,), 0, NUM_EXPERTS - 1)) % NUM_EXPERTS
    expert_ids = jnp.arange(NUM_EXPERTS)[None, :]
    extra_elig = jax.random.randint(k_elig, (BATCH, NUM_EXPERTS), 0, 8) == 0
    eligible = extra_elig | (expert_ids == first_choice[:, None]) | (expert_ids == second_choice[:, None])
    return first_choice.astype(jnp.int32), second_choice.astype(jnp.int32), eligible.astype(jnp.int32)


def setup_inputs(seed: int = 0) -> dict:
    keys = jax.random.split(jax.random.key(seed), 22)
    expert_one, expert_two, eligible = draw_routes(keys[0])
    value_mean = jax.random.normal(keys[3], (BATCH, 1, NUM_KV_HEADS, HEAD_DIM), jnp.float32)
    value_draw = jax.random.normal(keys[4], (BATCH, SEQ_LEN, NUM_KV_HEADS, HEAD_DIM), jnp.float32)
    ln1_gain = (1.0 + 0.3 * jax.random.normal(keys[6], (D_MODEL,), jnp.float32)).astype(jnp.bfloat16)
    ln2_gain = (1.0 + 0.3 * jax.random.normal(keys[16], (D_MODEL,), jnp.float32)).astype(jnp.bfloat16)
    return {
        'tokens': draw_normal(keys[1], (BATCH, D_MODEL), 1.0),
        'k_cache': draw_normal(keys[2], (BATCH, SEQ_LEN, NUM_KV_HEADS, HEAD_DIM), 2.0),
        'v_cache': (value_draw + value_mean).astype(jnp.bfloat16),
        'positions': draw_positions(keys[5]),
        'expert_one': expert_one,
        'expert_two': expert_two,
        'eligible': eligible,
        'ln1_gain': ln1_gain,
        'ln1_bias': draw_normal(keys[7], (D_MODEL,), 0.3),
        'w_query': draw_normal(keys[8], (D_MODEL, Q_DIM), D_MODEL ** -0.5),
        'b_query': draw_normal(keys[9], (Q_DIM,), 0.5),
        'w_key': draw_normal(keys[10], (D_MODEL, KV_DIM), D_MODEL ** -0.5),
        'b_key': draw_normal(keys[11], (KV_DIM,), 0.5),
        'w_value': draw_normal(keys[12], (D_MODEL, KV_DIM), D_MODEL ** -0.5),
        'b_value': draw_normal(keys[13], (KV_DIM,), 0.5),
        'w_out': draw_normal(keys[14], (Q_DIM, D_MODEL), Q_DIM ** -0.5),
        'b_out': draw_normal(keys[15], (D_MODEL,), 0.3),
        'ln2_gain': ln2_gain,
        'ln2_bias': draw_normal(keys[17], (D_MODEL,), 0.3),
        'w_router': draw_normal(keys[18], (D_MODEL, NUM_EXPERTS), D_MODEL ** -0.5),
        'w_gate': draw_normal(keys[19], (NUM_EXPERTS, D_MODEL, FF_DIM), D_MODEL ** -0.5),
        'w_up': draw_normal(keys[20], (NUM_EXPERTS, D_MODEL, FF_DIM), D_MODEL ** -0.5),
        'w_down': draw_normal(keys[21], (NUM_EXPERTS, FF_DIM, D_MODEL), FF_DIM ** -0.5),
    }


def layer_norm(values_in, gain, bias):
    mean_val = jnp.mean(values_in, axis=-1, keepdims=True)
    centered = values_in - mean_val
    var_val = jnp.mean(centered * centered, axis=-1, keepdims=True)
    return centered * lax.rsqrt(var_val + LN_EPS) * gain.astype(jnp.float32) + bias.astype(jnp.float32)


def rope_tables(positions):
    half_dim = HEAD_DIM // 2
    inv_freq = ROPE_BASE ** (jnp.arange(half_dim, dtype=jnp.float32) * (-2.0 / HEAD_DIM))
    angles = positions.astype(jnp.float32)[:, None] * inv_freq[None, :]
    angles = jnp.concatenate([angles, angles], axis=-1)
    return jnp.cos(angles), jnp.sin(angles)


def apply_rope(values_in, cos_tab, sin_tab):
    half_dim = values_in.shape[-1] // 2
    rotated = jnp.concatenate([-values_in[..., half_dim:], values_in[..., :half_dim]], axis=-1)
    return values_in * cos_tab[:, None, :] + rotated * sin_tab[:, None, :]


def attend_one(seq_parts):
    q_seq, k_seq, v_seq, k_one, v_one, pos_one = seq_parts
    score_scale = HEAD_DIM ** -0.5
    q_f = q_seq.astype(jnp.float32)
    s_cache = jnp.einsum('kgd,skd->kgs', q_f, k_seq.astype(jnp.float32)) * score_scale
    valid_mask = jnp.arange(SEQ_LEN)[None, None, :] < pos_one
    s_cache = jnp.where(valid_mask, s_cache, -jnp.inf)
    s_new = jnp.einsum('kgd,kd->kg', q_f, k_one.astype(jnp.float32)) * score_scale
    top_val = jnp.maximum(jnp.max(s_cache, axis=-1), s_new)
    e_cache = jnp.exp(s_cache - top_val[..., None])
    e_new = jnp.exp(s_new - top_val)
    denom_sum = jnp.sum(e_cache, axis=-1) + e_new
    p_cache = (e_cache / denom_sum[..., None]).astype(jnp.bfloat16).astype(jnp.float32)
    p_new = (e_new / denom_sum).astype(jnp.bfloat16).astype(jnp.float32)
    attn_vals = jnp.einsum('kgs,skd->kgd', p_cache, v_seq.astype(jnp.float32))
    return attn_vals + p_new[..., None] * v_one.astype(jnp.float32)[:, None, :]


def router_gates(h_two, w_router, expert_one, expert_two, eligible):
    logits = jnp.dot(h_two, w_router, preferred_element_type=jnp.float32)
    expert_ids = jnp.arange(NUM_EXPERTS)[None, :]
    hit_one = expert_ids == expert_one[:, None]
    hit_two = expert_ids == expert_two[:, None]
    keep_one = eligible == 1
    keep_two = keep_one & jnp.logical_not(hit_one)
    prob_one = jax.nn.softmax(jnp.where(keep_one, logits, -jnp.inf), axis=-1)
    prob_two = jax.nn.softmax(jnp.where(keep_two, logits, -jnp.inf), axis=-1)
    gate_one = jnp.sum(jnp.where(hit_one, prob_one, 0.0), axis=-1)
    gate_two = jnp.sum(jnp.where(hit_two, prob_two, 0.0), axis=-1)
    return gate_one, gate_two


def reference(tokens, k_cache, v_cache, positions, expert_one, expert_two, eligible, ln1_gain, ln1_bias, w_query, b_query, w_key, b_key, w_value, b_value, w_out, b_out, ln2_gain, ln2_bias, w_router, w_gate, w_up, w_down):
    x_f = tokens.astype(jnp.float32)
    h_one = layer_norm(x_f, ln1_gain, ln1_bias).astype(jnp.bfloat16)
    cos_tab, sin_tab = rope_tables(positions)
    q_lin = jnp.dot(h_one, w_query, preferred_element_type=jnp.float32) + b_query.astype(jnp.float32)
    q_rot = apply_rope(q_lin.reshape(BATCH, NUM_HEADS, HEAD_DIM), cos_tab, sin_tab).astype(jnp.bfloat16)
    k_lin = jnp.dot(h_one, w_key, preferred_element_type=jnp.float32) + b_key.astype(jnp.float32)
    key_new = apply_rope(k_lin.reshape(BATCH, NUM_KV_HEADS, HEAD_DIM), cos_tab, sin_tab).astype(jnp.bfloat16)
    v_lin = jnp.dot(h_one, w_value, preferred_element_type=jnp.float32) + b_value.astype(jnp.float32)
    value_new = v_lin.astype(jnp.bfloat16).reshape(BATCH, NUM_KV_HEADS, HEAD_DIM)
    q_grp = q_rot.reshape(BATCH, NUM_KV_HEADS, GROUP_SIZE, HEAD_DIM)
    attn_vals = lax.map(attend_one, (q_grp, k_cache, v_cache, key_new, value_new, positions))
    attn_flat = attn_vals.astype(jnp.bfloat16).reshape(BATCH, Q_DIM)
    x_mid = (x_f + jnp.dot(attn_flat, w_out, preferred_element_type=jnp.float32) + b_out.astype(jnp.float32)).astype(jnp.bfloat16)
    h_two = layer_norm(x_mid.astype(jnp.float32), ln2_gain, ln2_bias).astype(jnp.bfloat16)
    gate_one, gate_two = router_gates(h_two, w_router, expert_one, expert_two, eligible)

    def expert_step(acc_sum, expert_parts):
        gate_w, up_w, down_w, expert_idx = expert_parts
        u_val = jnp.dot(h_two, gate_w, preferred_element_type=jnp.float32)
        v_val = jnp.dot(h_two, up_w, preferred_element_type=jnp.float32)
        z_val = (jax.nn.silu(u_val) * v_val).astype(jnp.bfloat16)
        out_val = jnp.dot(z_val, down_w, preferred_element_type=jnp.float32).astype(jnp.bfloat16)
        weight_col = jnp.where(expert_one == expert_idx, gate_one, 0.0) + jnp.where(expert_two == expert_idx, gate_two, 0.0)
        return acc_sum + weight_col[:, None] * out_val.astype(jnp.float32), None

    y_sum, _ = lax.scan(expert_step, jnp.zeros((BATCH, D_MODEL), jnp.float32), (w_gate, w_up, w_down, jnp.arange(NUM_EXPERTS)))
    tokens_out = (x_mid.astype(jnp.float32) + y_sum).astype(jnp.bfloat16)
    return tokens_out, key_new, value_new
```

```python
import functools

import jax
import jax.numpy as jnp
from jax import lax
from jax.experimental import pallas as pl
from jax.experimental.pallas import tpu as pltpu
from jax.sharding import PartitionSpec as P

ROPE_BASE = 10000.0
LN_EPS = 1e-5
VMEM_CAP = 60 * 1024 * 1024
F32 = jnp.float32
BF16 = jnp.bfloat16


def layer_norm(values_in, gain, bias):
    mean_val = jnp.mean(values_in, axis=-1, keepdims=True)
    centered = values_in - mean_val
    var_val = jnp.mean(centered * centered, axis=-1, keepdims=True)
    return centered * lax.rsqrt(var_val + LN_EPS) * gain.astype(F32) + bias.astype(F32)


def rope_tables(positions, head_dim):
    half_dim = head_dim // 2
    inv_freq = ROPE_BASE ** (jnp.arange(half_dim, dtype=F32) * (-2.0 / head_dim))
    angles = positions.astype(F32)[:, None] * inv_freq[None, :]
    cos_half, sin_half = jnp.cos(angles), jnp.sin(angles)
    return jnp.concatenate([cos_half, cos_half], axis=-1), jnp.concatenate([-sin_half, sin_half], axis=-1)


def qkv_kernel(heads, x_ref, gain_ref, bias_ref, cos_ref, sin_ref, wq_ref, wk_ref, wv_ref, bq_ref, bk_ref, bv_ref,
               q_out, k_out, v_out, h_scr, q_scr, k_scr, v_scr):
    step = pl.program_id(0)
    toks = x_ref.shape[0]
    hd = cos_ref.shape[1]

    @pl.when(step == 0)
    def _():
        h_scr[...] = layer_norm(x_ref[...].astype(F32), gain_ref[...], bias_ref[...]).astype(BF16)

    h_one = h_scr[...]
    per_step = wq_ref.shape[1] // hd
    for w_ref, b_ref, scr, rotate in ((wq_ref, bq_ref, q_scr, True), (wk_ref, bk_ref, k_scr, True), (wv_ref, bv_ref, v_scr, False)):
        lin = jnp.dot(h_one, w_ref[...], preferred_element_type=F32) + b_ref[...].astype(F32)
        for sub in range(per_step):
            part = lin[:, sub * hd:(sub + 1) * hd]
            if rotate:
                part = part * cos_ref[...] + pltpu.roll(part, hd // 2, 1) * sin_ref[...]
            scr[pl.ds(step * per_step + sub, toks, stride=heads), :] = part

    @pl.when(step == pl.num_programs(0) - 1)
    def _():
        for scr, out in ((q_scr, q_out), (k_scr, k_out), (v_scr, v_out)):
            out[...] = scr[...].astype(BF16)


def qkv_project(tokens, gain, bias, cos_tab, sin_tab, wq, bq, wk, bk, wv, bv):
    toks, d_model = tokens.shape
    hd = cos_tab.shape[1]
    heads = wq.shape[1] // hd
    tile = 256
    full = lambda shape: pl.BlockSpec(shape, lambda i: (0,) * len(shape))
    w_spec = pl.BlockSpec((d_model, tile), lambda i: (0, i))
    b_spec = pl.BlockSpec((1, tile), lambda i: (0, i))
    out = jax.ShapeDtypeStruct((toks * heads, hd), BF16)
    row = lambda v: v.reshape(1, -1)
    return pl.pallas_call(
        functools.partial(qkv_kernel, heads),
        grid=(wq.shape[1] // tile,),
        in_specs=[full((toks, d_model)), full((1, d_model)), full((1, d_model)), full((toks, hd)), full((toks, hd)),
                  w_spec, w_spec, w_spec, b_spec, b_spec, b_spec],
        out_specs=[full((toks * heads, hd))] * 3,
        out_shape=[out] * 3,
        scratch_shapes=[pltpu.VMEM((toks, d_model), BF16)] + [pltpu.VMEM((toks * heads, hd), F32)] * 3,
        compiler_params=pltpu.CompilerParams(dimension_semantics=("arbitrary",), vmem_limit_bytes=VMEM_CAP),
        cost_estimate=pl.CostEstimate(flops=6 * toks * d_model * wq.shape[1], bytes_accessed=6 * d_model * wq.shape[1], transcendentals=0),
        name="qkv_project",
    )(tokens, row(gain), row(bias), cos_tab, sin_tab, wq, wk, wv, row(bq), row(bk), row(bv))


def attend_kernel(pos_ref, q_ref, kn_ref, vn_ref, k_ref, v_ref, o_ref):
    blk, seq, heads, hd = k_ref.shape
    groups = 128 // heads
    scale = hd ** -0.5
    rows = seq // groups
    two = 2 * heads
    r_id = lax.broadcasted_iota(jnp.int32, (two, 128), 0)
    l_id = lax.broadcasted_iota(jnp.int32, (two, 128), 1)
    pick = (l_id // two == r_id // heads) & (l_id % heads == r_id % heads)
    diag = lax.broadcasted_iota(jnp.int32, (heads, 128), 1) % heads == lax.broadcasted_iota(jnp.int32, (heads, 128), 0)
    s_id = groups * lax.broadcasted_iota(jnp.int32, (rows, 128), 0) + lax.broadcasted_iota(jnp.int32, (rows, 128), 1) // heads
    zero_q = jnp.zeros((heads, hd), BF16)

    def all_groups(vals, op):
        vals = op(vals, pltpu.roll(vals, heads, 1))
        return op(vals, pltpu.roll(vals, 2 * heads, 1))

    for tok in range(blk):
        pos = pos_ref[pl.program_id(0) * blk + tok]
        q_tok = q_ref[tok]
        top = jnp.concatenate([q_tok, zero_q], axis=1)
        bot = jnp.concatenate([zero_q, q_tok], axis=1)
        q_mat = jnp.concatenate([top, bot, top, bot], axis=0)
        k_tok = k_ref[tok].reshape(seq // 2, 2, heads, hd)
        k_mat = jnp.concatenate([k_tok[:, 0].reshape(seq // 2 * heads, hd), k_tok[:, 1].reshape(seq // 2 * heads, hd)], axis=1)
        raw = lax.dot_general(k_mat, q_mat, (((1,), (1,)), ((), ())), preferred_element_type=F32)
        s_cache = jnp.sum(jnp.where(pick[None], raw.reshape(rows, two, 128), 0.0), axis=1) * scale
        s_cache = jnp.where(s_id < pos, s_cache, -jnp.inf)
        new_col = jnp.sum(q_tok.astype(F32) * kn_ref[tok].astype(F32), axis=1, keepdims=True)
        s_new = jnp.sum(jnp.where(diag, new_col, 0.0), axis=0, keepdims=True) * scale
        top_val = jnp.maximum(all_groups(jnp.max(s_cache, axis=0, keepdims=True), jnp.maximum), s_new)
        e_cache = jnp.exp(s_cache - top_val)
        e_new = jnp.exp(s_new - top_val)
        denom = all_groups(jnp.sum(e_cache, axis=0, keepdims=True), jnp.add) + e_new
        p_cache = e_cache / denom
        p_new = (e_new / denom).astype(BF16).astype(F32)
        p_mat = jnp.concatenate([jnp.where(diag, p_cache[r:r + 1, :], 0.0).astype(BF16) for r in range(rows)], axis=1)
        vals = jnp.dot(p_mat, v_ref[tok].reshape(seq * heads, hd), preferred_element_type=F32)
        p_col = jnp.sum(jnp.where(diag, p_new, 0.0), axis=1, keepdims=True) * (1.0 / groups)
        o_ref[tok] = vals + p_col * vn_ref[tok].astype(F32)


def attend(positions, q_rot, key_new, value_new, k_cache, v_cache):
    toks, seq, heads, hd = k_cache.shape
    blk = 4
    row = pl.BlockSpec((blk, heads, hd), lambda i, pos: (i, 0, 0))
    cache = pl.BlockSpec((blk, seq, heads, hd), lambda i, pos: (i, 0, 0, 0))
    return pl.pallas_call(
        attend_kernel,
        grid_spec=pltpu.PrefetchScalarGridSpec(
            num_scalar_prefetch=1, grid=(toks // blk,),
            in_specs=[row, row, row, cache, cache], out_specs=row),
        out_shape=jax.ShapeDtypeStruct((toks, heads, hd), F32),
        compiler_params=pltpu.CompilerParams(dimension_semantics=("arbitrary",), vmem_limit_bytes=VMEM_CAP),
        cost_estimate=pl.CostEstimate(flops=4 * toks * seq * heads * hd * 32, bytes_accessed=4 * toks * seq * heads * hd, transcendentals=0),
        name="attend",
    )(positions, q_rot, key_new, value_new, k_cache, v_cache)


def out_kernel(heads, x_ref, a_ref, w_ref, b_ref, gain_ref, bias_ref, wr_ref, e1_ref, e2_ref, el_ref,
               x1_out, h2_out, g_out, a_scr):
    step = pl.program_id(0)
    toks = x_ref.shape[0]
    hd = a_ref.shape[1]
    tile = w_ref.shape[1]

    @pl.when(step == 0)
    def _():
        for head in range(heads):
            a_scr[:, head * hd:(head + 1) * hd] = a_ref[pl.ds(head, toks, stride=heads), :].astype(BF16)

    cols = pl.ds(pl.multiple_of(step * tile, tile), tile)
    lin = jnp.dot(a_scr[...], w_ref[...], preferred_element_type=F32)
    x1_out[:, cols] = (x_ref[:, cols].astype(F32) + lin + b_ref[...].astype(F32)).astype(BF16)

    @pl.when(step == pl.num_programs(0) - 1)
    def _():
        h_two = layer_norm(x1_out[...].astype(F32), gain_ref[...], bias_ref[...]).astype(BF16)
        h2_out[...] = h_two
        logits = jnp.dot(h_two, wr_ref[...], preferred_element_type=F32)
        ids = lax.broadcasted_iota(jnp.int32, logits.shape, 1)
        hit_one, hit_two = ids == e1_ref[...], ids == e2_ref[...]
        keep_one = el_ref[...] == 1
        keep_two = keep_one & jnp.logical_not(hit_one)

        def prob(keep):
            masked = jnp.where(keep, logits, -jnp.inf)
            expd = jnp.exp(masked - jnp.max(masked, axis=1, keepdims=True))
            return expd / jnp.sum(expd, axis=1, keepdims=True)

        g_out[...] = jnp.where(hit_one, prob(keep_one), 0.0) + jnp.where(hit_two, prob(keep_two), 0.0)


def out_project(tokens, attn, w_out, b_out, gain, bias, w_router, e1, e2, eligible):
    toks, d_model = tokens.shape
    rows, hd = attn.shape
    tile = 256
    experts = w_router.shape[1]
    full = lambda shape: pl.BlockSpec(shape, lambda i: (0,) * len(shape))
    row = lambda v: v.reshape(1, -1)
    return pl.pallas_call(
        functools.partial(out_kernel, rows // toks),
        grid=(d_model // tile,),
        in_specs=[full((toks, d_model)), full((rows, hd)), pl.BlockSpec((w_out.shape[0], tile), lambda i: (0, i)),
                  pl.BlockSpec((1, tile), lambda i: (0, i)), full((1, d_model)), full((1, d_model)), full((d_model, experts)),
                  full((toks, 1)), full((toks, 1)), full((toks, experts))],
        out_specs=[full((toks, d_model)), full((toks, d_model)), full((toks, experts))],
        out_shape=[jax.ShapeDtypeStruct((toks, d_model), BF16), jax.ShapeDtypeStruct((toks, d_model), BF16),
                   jax.ShapeDtypeStruct((toks, experts), F32)],
        scratch_shapes=[pltpu.VMEM((toks, w_out.shape[0]), BF16)],
        compiler_params=pltpu.CompilerParams(dimension_semantics=("arbitrary",), vmem_limit_bytes=VMEM_CAP),
        cost_estimate=pl.CostEstimate(flops=2 * toks * d_model * d_model, bytes_accessed=2 * d_model * d_model, transcendentals=0),
        name="out_project",
    )(tokens, attn, w_out, row(b_out), row(gain), row(bias), w_router, e1[:, None], e2[:, None], eligible)


def expert_mlp(expert_in, w_gate, w_up, w_down):
    u_val = jnp.dot(expert_in, w_gate, preferred_element_type=F32)
    v_val = jnp.dot(expert_in, w_up, preferred_element_type=F32)
    z_val = (jax.nn.silu(u_val) * v_val).astype(BF16)
    return jnp.dot(z_val, w_down, preferred_element_type=F32).astype(BF16)


def solution(mesh):
    def local_step(tokens, k_cache, v_cache, positions, expert_one, expert_two, eligible, ln1_gain, ln1_bias, w_query, b_query, w_key, b_key, w_value, b_value, w_out, b_out, ln2_gain, ln2_bias, w_router, w_gate, w_up, w_down):
        toks, seq, heads, hd = k_cache.shape
        cos_tab, sin_tab = rope_tables(positions, hd)
        q_rot, key_new, value_new = (
            v.reshape(toks, heads, hd)
            for v in qkv_project(tokens, ln1_gain, ln1_bias, cos_tab, sin_tab, w_query, b_query, w_key, b_key, w_value, b_value))
        attn = attend(positions, q_rot, key_new, value_new, k_cache, v_cache)
        x_mid, h_two, gates = out_project(tokens, attn.reshape(toks * heads, hd), w_out, b_out, ln2_gain, ln2_bias, w_router, expert_one, expert_two, eligible)
        me = lax.axis_index('ep')
        gates_all = lax.all_gather(gates, 'ep', axis=0, tiled=True)
        h_all = lax.all_gather(h_two, 'ep', axis=0, tiled=True)
        mine = jnp.arange(gates.shape[1])[None, :] == me
        weight = jnp.sum(jnp.where(mine, gates_all, 0.0), axis=1, keepdims=True)
        expert_out = expert_mlp(h_all, w_gate[0], w_up[0], w_down[0])
        part = (weight * expert_out.astype(F32)).astype(BF16)
        y_sum = lax.psum_scatter(part, 'ep', scatter_dimension=0, tiled=True)
        tokens_out = (x_mid.astype(F32) + y_sum.astype(F32)).astype(BF16)
        return tokens_out, key_new, value_new

    row_spec = P('ep', None)
    cache_spec = P('ep', None, None, None)
    vec_spec = P('ep')
    rep_one = P(None)
    rep_two = P(None, None)
    expert_spec = P('ep', None, None)
    in_specs = (row_spec, cache_spec, cache_spec, vec_spec, vec_spec, vec_spec, row_spec, rep_one, rep_one, rep_two, rep_one, rep_two, rep_one, rep_two, rep_one, rep_two, rep_one, rep_one, rep_one, rep_two, expert_spec, expert_spec, expert_spec)
    out_specs = (row_spec, expert_spec, expert_spec)
    return jax.shard_map(local_step, mesh=mesh, in_specs=in_specs, out_specs=out_specs, check_vma=False)
```

```python
import functools

import jax
import jax.numpy as jnp
from jax import lax
from jax.experimental import pallas as pl
from jax.experimental.pallas import tpu as pltpu
from jax.sharding import PartitionSpec as P

ROPE_BASE = 10000.0
LN_EPS = 1e-5
VMEM_CAP = 60 * 1024 * 1024
F32 = jnp.float32
BF16 = jnp.bfloat16


def layer_norm(values_in, gain, bias):
    mean_val = jnp.mean(values_in, axis=-1, keepdims=True)
    centered = values_in - mean_val
    var_val = jnp.mean(centered * centered, axis=-1, keepdims=True)
    return centered * lax.rsqrt(var_val + LN_EPS) * gain.astype(F32) + bias.astype(F32)


def rope_tables(positions, head_dim):
    half_dim = head_dim // 2
    inv_freq = ROPE_BASE ** (jnp.arange(half_dim, dtype=F32) * (-2.0 / head_dim))
    angles = positions.astype(F32)[:, None] * inv_freq[None, :]
    cos_half, sin_half = jnp.cos(angles), jnp.sin(angles)
    return jnp.concatenate([cos_half, cos_half], axis=-1), jnp.concatenate([-sin_half, sin_half], axis=-1)


def qkv_kernel(heads, x_ref, vec_ref, cos_ref, sin_ref, wq_ref, wk_ref, wv_ref, q_out, k_out, v_out, h_scr, q_scr, k_scr, v_scr):
    step = pl.program_id(0)
    toks = x_ref.shape[0]
    hd = cos_ref.shape[1]
    tile = wq_ref.shape[1]

    @pl.when(step == 0)
    def _():
        h_scr[...] = layer_norm(x_ref[...].astype(F32), vec_ref[0:1, :], vec_ref[1:2, :]).astype(BF16)

    h_one = h_scr[...]
    cols = pl.ds(pl.multiple_of(step * tile, tile), tile)
    per_step = tile // hd
    for row, w_ref, scr in ((2, wq_ref, q_scr), (3, wk_ref, k_scr), (4, wv_ref, v_scr)):
        lin = jnp.dot(h_one, w_ref[...], preferred_element_type=F32) + vec_ref[row:row + 1, cols]
        for sub in range(per_step):
            part = lin[:, sub * hd:(sub + 1) * hd]
            if row < 4:
                part = part * cos_ref[...] + pltpu.roll(part, hd // 2, 1) * sin_ref[...]
            scr[pl.ds(step * per_step + sub, toks, stride=heads), :] = part

    @pl.when(step == pl.num_programs(0) - 1)
    def _():
        for scr, out in ((q_scr, q_out), (k_scr, k_out), (v_scr, v_out)):
            out[...] = scr[...].astype(BF16)


def full_spec(shape):
    return pl.BlockSpec(shape, lambda *ids: (0,) * len(shape))


def qkv_project(tokens, vecs, cos_tab, sin_tab, wq, wk, wv):
    toks, d_model = tokens.shape
    hd = cos_tab.shape[1]
    heads = wq.shape[1] // hd
    tile = 512
    w_spec = pl.BlockSpec((d_model, tile), lambda i: (0, i))
    out = jax.ShapeDtypeStruct((toks * heads, hd), BF16)
    return pl.pallas_call(
        functools.partial(qkv_kernel, heads),
        grid=(wq.shape[1] // tile,),
        in_specs=[full_spec((toks, d_model)), full_spec(vecs.shape), full_spec((toks, hd)), full_spec((toks, hd)), w_spec, w_spec, w_spec],
        out_specs=[full_spec((toks * heads, hd))] * 3,
        out_shape=[out] * 3,
        scratch_shapes=[pltpu.VMEM((toks, d_model), BF16)] + [pltpu.VMEM((toks * heads, hd), F32)] * 3,
        compiler_params=pltpu.CompilerParams(dimension_semantics=("arbitrary",), vmem_limit_bytes=VMEM_CAP),
        cost_estimate=pl.CostEstimate(flops=6 * toks * d_model * wq.shape[1], bytes_accessed=6 * d_model * wq.shape[1], transcendentals=0),
        name="qkv_project",
    )(tokens, vecs, cos_tab, sin_tab, wq, wk, wv)


def attend_kernel(pos_ref, q_ref, kn_ref, vn_ref, k_ref, v_ref, o_ref):
    blk, seq, heads, hd = k_ref.shape
    groups = 128 // heads
    scale = hd ** -0.5
    rows = seq // groups
    half = rows // 2
    two = 2 * heads
    r_id = lax.broadcasted_iota(jnp.int32, (two, 128), 0)
    l_id = lax.broadcasted_iota(jnp.int32, (two, 128), 1)
    pick = (l_id // two == r_id // heads) & (l_id % heads == r_id % heads)
    diag = lax.broadcasted_iota(jnp.int32, (heads, 128), 1) % heads == lax.broadcasted_iota(jnp.int32, (heads, 128), 0)
    s_id = groups * lax.broadcasted_iota(jnp.int32, (rows, 128), 0) + lax.broadcasted_iota(jnp.int32, (rows, 128), 1) // heads
    zero_q = jnp.zeros((heads, hd), BF16)

    def all_groups(vals, op):
        vals = op(vals, pltpu.roll(vals, heads, 1))
        return op(vals, pltpu.roll(vals, 2 * heads, 1))

    s_list = []
    for tok in range(blk):
        pos = pos_ref[pl.program_id(0) * blk + tok]
        q_tok = q_ref[tok]
        top = jnp.concatenate([q_tok, zero_q], axis=1)
        bot = jnp.concatenate([zero_q, q_tok], axis=1)
        q_mat = jnp.concatenate([top, bot, top, bot], axis=0)
        k_tok = k_ref[tok].reshape(seq // 2, 2, heads, hd)
        k_mat = jnp.concatenate([k_tok[:, 0].reshape(seq // 2 * heads, hd), k_tok[:, 1].reshape(seq // 2 * heads, hd)], axis=1)
        raw = lax.dot_general(k_mat, q_mat, (((1,), (1,)), ((), ())), preferred_element_type=F32)
        s_tok = jnp.sum(jnp.where(pick[None], raw.reshape(rows, two, 128), 0.0), axis=1) * scale
        s_list.append(jnp.where(s_id < pos, s_tok, -jnp.inf)[None])
    s_cache = jnp.concatenate(s_list, axis=0)
    new_col = jnp.sum(q_ref[...].astype(F32) * kn_ref[...].astype(F32), axis=2, keepdims=True)
    s_new = jnp.sum(jnp.where(diag[None], new_col, 0.0), axis=1) * scale
    top_val = jnp.maximum(all_groups(jnp.max(s_cache, axis=1), jnp.maximum), s_new)
    e_cache = jnp.exp(s_cache - top_val[:, None, :])
    e_new = jnp.exp(s_new - top_val)
    denom = all_groups(jnp.sum(e_cache, axis=1), jnp.add) + e_new
    p_cache = e_cache / denom[:, None, :]
    p_new = (e_new / denom).astype(BF16).astype(F32)
    lane_id = lax.broadcasted_iota(jnp.int32, (heads, 128), 1)
    once = diag & (lane_id < heads)
    p_col = jnp.sum(jnp.where(once[None], p_new[:, None, :], 0.0), axis=2, keepdims=True)
    for tok in range(blk):
        p_rows = [jnp.where(diag, p_cache[tok, r:r + 1, :], 0.0).astype(BF16) for r in range(rows)]
        p_mat = jnp.concatenate([jnp.concatenate(p_rows[:half], axis=1), jnp.concatenate(p_rows[half:], axis=1)], axis=0)
        v_tok = v_ref[tok].reshape(2, seq // 2 * heads, hd)
        v_mat = jnp.concatenate([v_tok[0], v_tok[1]], axis=1)
        vals = jnp.dot(p_mat, v_mat, preferred_element_type=F32)
        o_ref[tok] = vals[:heads, :hd] + vals[heads:, hd:] + p_col[tok] * vn_ref[tok].astype(F32)


def attend(positions, q_rot, key_new, value_new, k_cache, v_cache):
    toks, seq, heads, hd = k_cache.shape
    blk = 8
    row = pl.BlockSpec((blk, heads, hd), lambda i, pos: (i, 0, 0))
    cache = pl.BlockSpec((blk, seq, heads, hd), lambda i, pos: (i, 0, 0, 0))
    return pl.pallas_call(
        attend_kernel,
        grid_spec=pltpu.PrefetchScalarGridSpec(
            num_scalar_prefetch=1, grid=(toks // blk,),
            in_specs=[row, row, row, cache, cache], out_specs=row),
        out_shape=jax.ShapeDtypeStruct((toks, heads, hd), F32),
        compiler_params=pltpu.CompilerParams(dimension_semantics=("arbitrary",), vmem_limit_bytes=VMEM_CAP),
        cost_estimate=pl.CostEstimate(flops=4 * toks * seq * heads * hd * 32, bytes_accessed=4 * toks * seq * heads * hd, transcendentals=0),
        name="attend",
    )(positions, q_rot, key_new, value_new, k_cache, v_cache)


def out_kernel(heads, x_ref, a_ref, w_ref, vec_ref, wr_ref, route_ref, x1_out, h2_out, g_out, a_scr):
    step = pl.program_id(0)
    toks = x_ref.shape[0]
    hd = a_ref.shape[1]
    tile = w_ref.shape[1]
    experts = wr_ref.shape[0]

    @pl.when(step == 0)
    def _():
        for head in range(heads):
            a_scr[:, head * hd:(head + 1) * hd] = a_ref[pl.ds(head, toks, stride=heads), :].astype(BF16)

    cols = pl.ds(pl.multiple_of(step * tile, tile), tile)
    lin = jnp.dot(a_scr[...], w_ref[...], preferred_element_type=F32)
    x1_out[:, cols] = (x_ref[:, cols].astype(F32) + lin + vec_ref[5:6, cols]).astype(BF16)

    @pl.when(step == pl.num_programs(0) - 1)
    def _():
        h_two = layer_norm(x1_out[...].astype(F32), vec_ref[6:7, :], vec_ref[7:8, :]).astype(BF16)
        h2_out[...] = h_two
        logits = lax.dot_general(wr_ref[...], h_two, (((1,), (1,)), ((), ())), preferred_element_type=F32)
        ids = lax.broadcasted_iota(jnp.int32, logits.shape, 0)
        hit_one, hit_two = ids == route_ref[0:1, :], ids == route_ref[1:2, :]
        keep_one = route_ref[8:8 + experts, :] == 1
        keep_two = keep_one & jnp.logical_not(hit_one)

        def prob(keep):
            masked = jnp.where(keep, logits, -jnp.inf)
            expd = jnp.exp(masked - jnp.max(masked, axis=0, keepdims=True))
            return expd / jnp.sum(expd, axis=0, keepdims=True)

        g_out[...] = jnp.where(hit_one, prob(keep_one), 0.0) + jnp.where(hit_two, prob(keep_two), 0.0)


def out_project(tokens, attn, w_out, vecs, w_router_t, routes):
    toks, d_model = tokens.shape
    rows, hd = attn.shape
    tile = 512
    experts = w_router_t.shape[0]
    return pl.pallas_call(
        functools.partial(out_kernel, rows // toks),
        grid=(d_model // tile,),
        in_specs=[full_spec((toks, d_model)), full_spec((rows, hd)), pl.BlockSpec((w_out.shape[0], tile), lambda i: (0, i)),
                  full_spec(vecs.shape), full_spec((experts, d_model)), full_spec(routes.shape)],
        out_specs=[full_spec((toks, d_model)), full_spec((toks, d_model)), full_spec((experts, toks))],
        out_shape=[jax.ShapeDtypeStruct((toks, d_model), BF16), jax.ShapeDtypeStruct((toks, d_model), BF16),
                   jax.ShapeDtypeStruct((experts, toks), F32)],
        scratch_shapes=[pltpu.VMEM((toks, w_out.shape[0]), BF16)],
        compiler_params=pltpu.CompilerParams(dimension_semantics=("arbitrary",), vmem_limit_bytes=VMEM_CAP),
        cost_estimate=pl.CostEstimate(flops=2 * toks * d_model * d_model, bytes_accessed=2 * d_model * d_model, transcendentals=0),
        name="out_project",
    )(tokens, attn, w_out, vecs, w_router_t, routes)


def peer(me, flip):
    for bit in (1, 2, 4):
        if flip & bit:
            me = me + bit - 2 * bit * lax.rem(me // bit, 2)
    return me


PIECE = {(0, 0): 0, (0, 1): 1, (1, 0): 2, (1, 1): 3,
         (2, 0): 4, (4, 1): 5, (3, 0): 6, (5, 1): 7,
         (2, 1): 8, (4, 0): 9, (3, 1): 10, (5, 0): 11,
         (6, 0): 12, (6, 1): 13, (7, 0): 14, (7, 1): 15}


def moe_kernel(h_ref, gate_ref, x_ref, wg_hbm, wu_hbm, wd_hbm, out_ref,
               wg, wu, wd, hbuf, gates, wcol, zt_scr, z_scr, mine, first, dsend, drecv, yrecv, local_sem, send_sem, recv_sem):
    me = lax.axis_index('ep')
    toks, d_model = h_ref.shape
    ff = wg.shape[0]
    part = toks // 2
    parts = 4

    own = pltpu.make_async_copy(h_ref, hbuf.at[pl.ds(0, toks)], local_sem.at[0])
    own.start()
    loads = []
    for hbm, scr in ((wg_hbm, wg), (wu_hbm, wu), (wd_hbm, wd)):
        size = ff // 2
        for piece in range(2):
            rows = pl.ds(piece * size, size)
            loads.append(pltpu.make_async_copy(hbm.at[rows], scr.at[rows], local_sem.at[1 + len(loads)]))

    barrier = pltpu.get_barrier_semaphore()
    for flip in range(1, 8):
        pl.semaphore_signal(barrier, inc=1, device_id=(peer(me, flip),), device_id_type=pl.DeviceIdType.MESH)
    pl.semaphore_wait(barrier, 7)

    def remote(num, src, dst, flip):
        return pltpu.make_async_remote_copy(src_ref=src, dst_ref=dst, send_sem=send_sem.at[num], recv_sem=recv_sem.at[num],
                                            device_id=(peer(me, flip),), device_id_type=pl.DeviceIdType.MESH)

    def piece(flip, half):
        return hbuf.at[pl.ds(PIECE[(flip, half)] * part, part)]

    def pass_on(num, source, half, flip):
        return remote(num, piece(source, half), piece(source ^ flip, half), flip)

    sends = {}
    for num, half, flip in ((0, 0, 2), (3, 1, 4), (1, 1, 2), (2, 0, 4)):
        sends[num] = pass_on(num, 0, half, flip)
    sends[4] = remote(4, hbuf.at[pl.ds(0, toks)], hbuf.at[pl.ds(toks, toks)], 1)
    for num, source, half, flip in ((5, 2, 0, 4), (6, 4, 1, 2), (7, 2, 0, 1), (8, 2, 1, 1), (9, 4, 0, 1), (10, 4, 1, 1), (11, 6, 0, 1), (12, 6, 1, 1)):
        sends[num] = pass_on(num, source, half, flip)
    for flip in range(1, 8):
        sends[12 + flip] = remote(12 + flip, gate_ref, gates.at[flip], flip)
    for blk in range(4):
        sends[20 + blk] = remote(20 + blk, dsend.at[blk % 2], drecv.at[blk], 1)
    lower, upper = pl.ds(0, part), pl.ds(part, part)
    sends[24] = remote(24, drecv.at[1, lower], yrecv.at[0, lower], 2)
    sends[25] = remote(25, drecv.at[1, upper], yrecv.at[1, upper], 4)
    sends[26] = remote(26, drecv.at[2, lower], yrecv.at[0, upper], 2)
    sends[27] = remote(27, drecv.at[2, upper], yrecv.at[1, lower], 4)
    sends[28] = remote(28, drecv.at[3], yrecv.at[2], 6)

    own.wait()
    for num in (0, 3, 1, 2, 4):
        sends[num].start()
    for flip in range(1, 8):
        sends[12 + flip].start()
    for load in loads:
        load.start()
    gates[0] = gate_ref[...]
    for flip in range(1, 8):
        sends[12 + flip].wait_recv()
    same = lax.broadcasted_iota(jnp.int32, (toks, toks), 0) == lax.broadcasted_iota(jnp.int32, (toks, toks), 1)
    for flip in range(8):
        col = jnp.sum(jnp.where(same, gates[flip, pl.ds(me, 1), :], 0.0), axis=1, keepdims=True)
        for half in range(2):
            wcol[pl.ds(PIECE[(flip, half)] * part, part), :] = col[half * part:(half + 1) * part]

    def hidden(blk):
        size = ff // 2

        @pl.loop(0, 2)
        def _(idx):
            rows = pl.ds(pl.multiple_of(idx * size, 16), size)
            h_blk = hbuf[pl.ds(blk * 2 * toks, 2 * toks), :]
            nt = (((1,), (1,)), ((), ()))
            u_val = lax.dot_general(wg[rows, :], h_blk, nt, preferred_element_type=F32)
            v_val = lax.dot_general(wu[rows, :], h_blk, nt, preferred_element_type=F32)
            zt_scr[rows, :] = jax.nn.silu(u_val) * v_val

        z_scr[...] = zt_scr[...].T.astype(BF16)

    tile = 512

    def down(blk, first_row, store):
        rows = pl.ds(blk * 2 * toks + first_row, toks)

        @pl.loop(0, d_model // tile)
        def _(idx):
            cols = pl.ds(pl.multiple_of(idx * tile, tile), tile)
            val = jnp.dot(z_scr[pl.ds(first_row, toks), :], wd[:, cols], preferred_element_type=F32).astype(BF16)
            store(cols, wcol[rows, :] * val.astype(F32))

    def keep_theirs(blk):
        def store(cols, val):
            dsend[blk % 2, :, cols] = val.astype(BF16)
        return store

    def keep_mine(cols, val):
        mine[:, cols] = val

    def merge(blk):
        @pl.loop(0, d_model // tile)
        def _(idx):
            cols = pl.ds(pl.multiple_of(idx * tile, tile), tile)
            total = mine[:, cols] + drecv[blk, :, cols].astype(F32)
            if blk == 0:
                first[:, cols] = total
            else:
                drecv[blk, :, cols] = total.astype(BF16)

    def forward(arrived, nums):
        for num in arrived:
            sends[num].wait_recv()
        for num in nums:
            sends[num].start()

    forward((0, 3), (5, 6, 7, 10))
    for load in loads:
        load.wait()
    sends[4].wait_recv()
    homeward = {0: (), 1: (24, 25), 2: (26, 27), 3: (28,)}
    needs = {0: (), 1: (7, 10), 2: (8, 9), 3: (11, 12)}
    for blk in range(4):
        for num in needs[blk]:
            sends[num].wait_recv()
        hidden(blk)
        if blk == 0:
            forward((1, 2), (8, 9))
        if blk == 2:
            forward((5, 6), (11, 12))
        if blk >= 2:
            sends[18 + blk].wait_send()
        down(blk, toks, keep_theirs(blk))
        sends[20 + blk].start()
        down(blk, 0, keep_mine)
        sends[20 + blk].wait_recv()
        merge(blk)
        for num in homeward[blk]:
            sends[num].start()

    for num in range(24, 29):
        sends[num].wait_recv()

    @pl.loop(0, d_model // tile)
    def _(idx):
        cols = pl.ds(pl.multiple_of(idx * tile, tile), tile)
        total = first[:, cols] + yrecv[0, :, cols].astype(F32) + yrecv[1, :, cols].astype(F32) + yrecv[2, :, cols].astype(F32)
        out_ref[:, cols] = (x_ref[:, cols].astype(F32) + total).astype(BF16)

    for num in list(range(20)) + list(range(22, 29)):
        sends[num].wait_send()


def expert_exchange(h_two, gates, x_mid, w_gate_t, w_up_t, w_down):
    toks, d_model = h_two.shape
    ff = w_down.shape[0]
    experts = gates.shape[0]
    hbm = pl.BlockSpec(memory_space=pl.ANY)
    vmem = pl.BlockSpec(memory_space=pltpu.VMEM)
    return pl.pallas_call(
        moe_kernel,
        in_specs=[hbm, vmem, vmem, hbm, hbm, hbm],
        out_specs=vmem,
        out_shape=jax.ShapeDtypeStruct((toks, d_model), BF16),
        scratch_shapes=[
            pltpu.VMEM((ff, d_model), BF16), pltpu.VMEM((ff, d_model), BF16), pltpu.VMEM((ff, d_model), BF16),
            pltpu.VMEM((8 * toks, d_model), BF16),
            pltpu.VMEM((8, experts, toks), F32),
            pltpu.VMEM((8 * toks, 1), F32),
            pltpu.VMEM((ff, 2 * toks), F32),
            pltpu.VMEM((2 * toks, ff), BF16),
            pltpu.VMEM((toks, d_model), F32),
            pltpu.VMEM((toks, d_model), F32),
            pltpu.VMEM((2, toks, d_model), BF16),
            pltpu.VMEM((4, toks, d_model), BF16),
            pltpu.VMEM((3, toks, d_model), BF16),
            pltpu.SemaphoreType.DMA((7,)),
            pltpu.SemaphoreType.DMA((29,)),
            pltpu.SemaphoreType.DMA((29,)),
        ],
        compiler_params=pltpu.CompilerParams(collective_id=0, has_side_effects=True, vmem_limit_bytes=67043328),
        cost_estimate=pl.CostEstimate(flops=48 * toks * d_model * ff, bytes_accessed=6 * d_model * ff, transcendentals=0),
        name="expert_exchange",
    )(h_two, gates, x_mid, w_gate_t, w_up_t, w_down)


def solution(mesh):
    def local_step(tokens, k_cache, v_cache, positions, expert_one, expert_two, eligible, ln1_gain, ln1_bias, w_query, b_query, w_key, b_key, w_value, b_value, w_out, b_out, ln2_gain, ln2_bias, w_router, w_gate, w_up, w_down):
        toks, seq, heads, hd = k_cache.shape
        cos_tab, sin_tab = rope_tables(positions, hd)
        vecs = jnp.concatenate([ln1_gain, ln1_bias, b_query, b_key, b_value, b_out, ln2_gain, ln2_bias]).reshape(8, -1).astype(F32)
        pad = jnp.zeros((6, toks), jnp.int32)
        routes = jnp.concatenate([expert_one[None], expert_two[None], pad, eligible.T], axis=0)
        q_rot, key_new, value_new = (v.reshape(toks, heads, hd) for v in qkv_project(tokens, vecs, cos_tab, sin_tab, w_query, w_key, w_value))
        attn = attend(positions, q_rot, key_new, value_new, k_cache, v_cache)
        x_mid, h_two, gates = out_project(tokens, attn.reshape(toks * heads, hd), w_out, vecs, w_router.T, routes)
        tokens_out = expert_exchange(h_two, gates, x_mid, w_gate[0].T, w_up[0].T, w_down[0])
        return tokens_out, key_new, value_new

    row_spec = P('ep', None)
    cache_spec = P('ep', None, None, None)
    vec_spec = P('ep')
    rep_one = P(None)
    rep_two = P(None, None)
    expert_spec = P('ep', None, None)
    in_specs = (row_spec, cache_spec, cache_spec, vec_spec, vec_spec, vec_spec, row_spec, rep_one, rep_one, rep_two, rep_one, rep_two, rep_one, rep_two, rep_one, rep_two, rep_one, rep_one, rep_one, rep_two, expert_spec, expert_spec, expert_spec)
    out_specs = (row_spec, expert_spec, expert_spec)
    return jax.shard_map(local_step, mesh=mesh, in_specs=in_specs, out_specs=out_specs, check_vma=False)
```

```python
import functools

import jax
import jax.numpy as jnp
from jax import lax
from jax.experimental import pallas as pl
from jax.experimental.pallas import tpu as pltpu
from jax.sharding import PartitionSpec as P

ROPE_BASE = 10000.0
LN_EPS = 1e-5
VMEM_CAP = 60 * 1024 * 1024
F32 = jnp.float32
BF16 = jnp.bfloat16


def layer_norm(values_in, gain, bias):
    mean_val = jnp.mean(values_in, axis=-1, keepdims=True)
    centered = values_in - mean_val
    var_val = jnp.mean(centered * centered, axis=-1, keepdims=True)
    return centered * lax.rsqrt(var_val + LN_EPS) * gain.astype(F32) + bias.astype(F32)


def rope_tables(positions, head_dim):
    half_dim = head_dim // 2
    inv_freq = ROPE_BASE ** (jnp.arange(half_dim, dtype=F32) * (-2.0 / head_dim))
    angles = positions.astype(F32)[:, None] * inv_freq[None, :]
    cos_half, sin_half = jnp.cos(angles), jnp.sin(angles)
    return jnp.concatenate([cos_half, cos_half], axis=-1), jnp.concatenate([-sin_half, sin_half], axis=-1)


def ring(step, steps, depth, copies):
    @pl.when(step == 0)
    def _():
        for idx in range(depth - 1):
            for copy in copies(idx):
                copy.start()

    @pl.when(step + depth - 1 < steps)
    def _():
        for copy in copies(step + depth - 1):
            copy.start()

    for copy in copies(step):
        copy.wait()


def column_copies(hbms, bufs, sems, tile, depth):
    def copies(idx):
        slot = lax.rem(idx, depth) if not isinstance(idx, int) else idx % depth
        start = pl.multiple_of(idx * tile, tile) if not isinstance(idx, int) else idx * tile
        return [pltpu.make_async_copy(hbm.at[:, pl.ds(start, tile)], buf.at[slot], sems.at[num, slot])
                for num, (hbm, buf) in enumerate(zip(hbms, bufs))]
    return copies


def as_row(dst, row, vec_ref):
    width = vec_ref.shape[1]
    vals = vec_ref[...].astype(F32)
    for idx in range(vec_ref.shape[0]):
        dst[row:row + 1, idx * width:(idx + 1) * width] = vals[idx:idx + 1, :]


def qkv_kernel(heads, x_ref, g_ref, b_ref, bq_ref, bk_ref, bv_ref, cos_ref, sin_ref, wq_hbm, wk_hbm, wv_hbm, q_out, k_out, v_out,
               h_scr, q_scr, k_scr, v_scr, vec_ref, wq_buf, wk_buf, wv_buf, sems):
    step = pl.program_id(0)
    toks = x_ref.shape[0]
    hd = cos_ref.shape[1]
    depth, _, tile = wq_buf.shape
    slot = lax.rem(step, depth)
    ring(step, pl.num_programs(0), depth, column_copies((wq_hbm, wk_hbm, wv_hbm), (wq_buf, wk_buf, wv_buf), sems, tile, depth))

    @pl.when(step == 0)
    def _():
        for row, ref in enumerate((g_ref, b_ref, bq_ref, bk_ref, bv_ref)):
            as_row(vec_ref, row, ref)
        h_scr[...] = layer_norm(x_ref[...].astype(F32), vec_ref[0:1, :], vec_ref[1:2, :]).astype(BF16)

    h_one = h_scr[...]
    cols = pl.ds(pl.multiple_of(step * tile, tile), tile)
    per_step = tile // hd
    for row, w_buf, scr in ((2, wq_buf, q_scr), (3, wk_buf, k_scr), (4, wv_buf, v_scr)):
        lin = jnp.dot(h_one, w_buf[slot], preferred_element_type=F32) + vec_ref[row:row + 1, cols]
        for sub in range(per_step):
            part = lin[:, sub * hd:(sub + 1) * hd]
            if row < 4:
                part = part * cos_ref[...] + pltpu.roll(part, hd // 2, 1) * sin_ref[...]
            scr[pl.ds(step * per_step + sub, toks, stride=heads), :] = part

    @pl.when(step == pl.num_programs(0) - 1)
    def _():
        for scr, out in ((q_scr, q_out), (k_scr, k_out), (v_scr, v_out)):
            out[...] = scr[...].astype(BF16)


def full_spec(shape):
    return pl.BlockSpec(shape, lambda *ids: (0,) * len(shape))


def qkv_project(tokens, rows, cos_tab, sin_tab, wq, wk, wv):
    toks, d_model = tokens.shape
    hd = cos_tab.shape[1]
    heads = wq.shape[1] // hd
    tile, depth = 256, 4
    w_spec = pl.BlockSpec(memory_space=pl.ANY)
    out = jax.ShapeDtypeStruct((toks * heads, hd), BF16)
    return pl.pallas_call(
        functools.partial(qkv_kernel, heads),
        grid=(wq.shape[1] // tile,),
        in_specs=[full_spec((toks, d_model))] + [full_spec(row.shape) for row in rows] + [full_spec((toks, hd)), full_spec((toks, hd)), w_spec, w_spec, w_spec],
        out_specs=[full_spec((toks * heads, hd))] * 3,
        out_shape=[out] * 3,
        scratch_shapes=[pltpu.VMEM((toks, d_model), BF16)] + [pltpu.VMEM((toks * heads, hd), F32)] * 3
        + [pltpu.VMEM((8, d_model), F32)] + [pltpu.VMEM((depth, d_model, tile), BF16)] * 3 + [pltpu.SemaphoreType.DMA((3, depth))],
        compiler_params=pltpu.CompilerParams(dimension_semantics=("arbitrary",), vmem_limit_bytes=VMEM_CAP),
        cost_estimate=pl.CostEstimate(flops=6 * toks * d_model * wq.shape[1], bytes_accessed=6 * d_model * wq.shape[1], transcendentals=0),
        name="qkv_project",
    )(tokens, *rows, cos_tab, sin_tab, wq, wk, wv)


def attend_kernel(pos_ref, q_ref, kn_ref, vn_ref, k_hbm, v_hbm, o_ref, k_buf, v_buf, sems):
    depth, blk, seq, heads, hd = k_buf.shape
    step = pl.program_id(0)

    def copies(idx):
        slot = lax.rem(idx, depth) if not isinstance(idx, int) else idx % depth
        return [pltpu.make_async_copy(hbm.at[pl.ds(idx * blk, blk)], buf.at[slot], sems.at[num, slot])
                for num, (hbm, buf) in enumerate(((k_hbm, k_buf), (v_hbm, v_buf)))]

    ring(step, pl.num_programs(0), depth, copies)
    k_ref, v_ref = k_buf.at[lax.rem(step, depth)], v_buf.at[lax.rem(step, depth)]
    groups = 128 // heads
    scale = hd ** -0.5
    rows = seq // groups
    half = rows // 2
    two = 2 * heads
    r_id = lax.broadcasted_iota(jnp.int32, (two, 128), 0)
    l_id = lax.broadcasted_iota(jnp.int32, (two, 128), 1)
    pick = (l_id // two == r_id // heads) & (l_id % heads == r_id % heads)
    diag = lax.broadcasted_iota(jnp.int32, (heads, 128), 1) % heads == lax.broadcasted_iota(jnp.int32, (heads, 128), 0)
    s_id = groups * lax.broadcasted_iota(jnp.int32, (rows, 128), 0) + lax.broadcasted_iota(jnp.int32, (rows, 128), 1) // heads
    zero_q = jnp.zeros((heads, hd), BF16)

    def all_groups(vals, op):
        vals = op(vals, pltpu.roll(vals, heads, 1))
        return op(vals, pltpu.roll(vals, 2 * heads, 1))

    s_list = []
    for tok in range(blk):
        pos = pos_ref[pl.program_id(0) * blk + tok]
        q_tok = q_ref[tok]
        top = jnp.concatenate([q_tok, zero_q], axis=1)
        bot = jnp.concatenate([zero_q, q_tok], axis=1)
        q_mat = jnp.concatenate([top, bot, top, bot], axis=0)
        k_tok = k_ref[tok].reshape(seq // 2, 2, heads, hd)
        k_mat = jnp.concatenate([k_tok[:, 0].reshape(seq // 2 * heads, hd), k_tok[:, 1].reshape(seq // 2 * heads, hd)], axis=1)
        raw = lax.dot_general(k_mat, q_mat, (((1,), (1,)), ((), ())), preferred_element_type=F32)
        s_tok = jnp.sum(jnp.where(pick[None], raw.reshape(rows, two, 128), 0.0), axis=1) * scale
        s_list.append(jnp.where(s_id < pos, s_tok, -jnp.inf)[None])
    s_cache = jnp.concatenate(s_list, axis=0)
    new_col = jnp.sum(q_ref[...].astype(F32) * kn_ref[...].astype(F32), axis=2, keepdims=True)
    s_new = jnp.sum(jnp.where(diag[None], new_col, 0.0), axis=1) * scale
    top_val = jnp.maximum(all_groups(jnp.max(s_cache, axis=1), jnp.maximum), s_new)
    e_cache = jnp.exp(s_cache - top_val[:, None, :])
    e_new = jnp.exp(s_new - top_val)
    denom = all_groups(jnp.sum(e_cache, axis=1), jnp.add) + e_new
    p_cache = e_cache / denom[:, None, :]
    p_new = (e_new / denom).astype(BF16).astype(F32)
    lane_id = lax.broadcasted_iota(jnp.int32, (heads, 128), 1)
    once = diag & (lane_id < heads)
    p_col = jnp.sum(jnp.where(once[None], p_new[:, None, :], 0.0), axis=2, keepdims=True)
    for tok in range(blk):
        p_rows = [jnp.where(diag, p_cache[tok, r:r + 1, :], 0.0).astype(BF16) for r in range(rows)]
        p_mat = jnp.concatenate([jnp.concatenate(p_rows[:half], axis=1), jnp.concatenate(p_rows[half:], axis=1)], axis=0)
        v_tok = v_ref[tok].reshape(2, seq // 2 * heads, hd)
        v_mat = jnp.concatenate([v_tok[0], v_tok[1]], axis=1)
        vals = jnp.dot(p_mat, v_mat, preferred_element_type=F32)
        o_ref[tok] = vals[:heads, :hd] + vals[heads:, hd:] + p_col[tok] * vn_ref[tok].astype(F32)


def attend(positions, q_rot, key_new, value_new, k_cache, v_cache):
    toks, seq, heads, hd = k_cache.shape
    blk, depth = 8, 3
    row = pl.BlockSpec((blk, heads, hd), lambda i, pos: (i, 0, 0))
    cache = pl.BlockSpec(memory_space=pl.ANY)
    ring_buf = pltpu.VMEM((depth, blk, seq, heads, hd), BF16)
    return pl.pallas_call(
        attend_kernel,
        grid_spec=pltpu.PrefetchScalarGridSpec(
            num_scalar_prefetch=1, grid=(toks // blk,),
            in_specs=[row, row, row, cache, cache], out_specs=row,
            scratch_shapes=[ring_buf, ring_buf, pltpu.SemaphoreType.DMA((2, depth))]),
        out_shape=jax.ShapeDtypeStruct((toks, heads, hd), F32),
        compiler_params=pltpu.CompilerParams(dimension_semantics=("arbitrary",), vmem_limit_bytes=VMEM_CAP),
        cost_estimate=pl.CostEstimate(flops=4 * toks * seq * heads * hd * 32, bytes_accessed=4 * toks * seq * heads * hd, transcendentals=0),
        name="attend",
    )(positions, q_rot, key_new, value_new, k_cache, v_cache)


def out_kernel(heads, x_ref, a_ref, w_hbm, bo_ref, g_ref, b_ref, wr_ref, e1_ref, e2_ref, el_ref, x1_out, h2_out, g_out, a_scr, vec_ref, w_buf, sems):
    step = pl.program_id(0)
    toks = x_ref.shape[0]
    hd = a_ref.shape[1]
    depth, _, tile = w_buf.shape
    experts = wr_ref.shape[0]
    ring(step, pl.num_programs(0), depth, column_copies((w_hbm,), (w_buf,), sems, tile, depth))

    @pl.when(step == 0)
    def _():
        for row, ref in enumerate((bo_ref, g_ref, b_ref)):
            as_row(vec_ref, row, ref)
        for head in range(heads):
            a_scr[:, head * hd:(head + 1) * hd] = a_ref[pl.ds(head, toks, stride=heads), :].astype(BF16)

    cols = pl.ds(pl.multiple_of(step * tile, tile), tile)
    lin = jnp.dot(a_scr[...], w_buf[lax.rem(step, depth)], preferred_element_type=F32)
    x1_out[:, cols] = (x_ref[:, cols].astype(F32) + lin + vec_ref[0:1, cols]).astype(BF16)

    @pl.when(step == pl.num_programs(0) - 1)
    def _():
        h_two = layer_norm(x1_out[...].astype(F32), vec_ref[1:2, :], vec_ref[2:3, :]).astype(BF16)
        h2_out[...] = h_two
        logits = lax.dot_general(wr_ref[...], h_two, (((1,), (1,)), ((), ())), preferred_element_type=F32)
        ids = lax.broadcasted_iota(jnp.int32, logits.shape, 0)
        hit_one, hit_two = ids == e1_ref[...], ids == e2_ref[...]
        keep_one = el_ref[...] == 1
        keep_two = keep_one & jnp.logical_not(hit_one)

        def prob(keep):
            masked = jnp.where(keep, logits, -jnp.inf)
            expd = jnp.exp(masked - jnp.max(masked, axis=0, keepdims=True))
            return expd / jnp.sum(expd, axis=0, keepdims=True)

        g_out[...] = jnp.where(hit_one, prob(keep_one), 0.0) + jnp.where(hit_two, prob(keep_two), 0.0)


def out_project(tokens, attn, w_out, vec_rows, w_router_t, routes):
    toks, d_model = tokens.shape
    rows, hd = attn.shape
    tile, depth = 256, 6
    experts = w_router_t.shape[0]
    return pl.pallas_call(
        functools.partial(out_kernel, rows // toks),
        grid=(d_model // tile,),
        in_specs=[full_spec((toks, d_model)), full_spec((rows, hd)), pl.BlockSpec(memory_space=pl.ANY)]
        + [full_spec(row.shape) for row in vec_rows] + [full_spec((experts, d_model))] + [full_spec(route.shape) for route in routes],
        out_specs=[full_spec((toks, d_model)), full_spec((toks, d_model)), full_spec((experts, toks))],
        out_shape=[jax.ShapeDtypeStruct((toks, d_model), BF16), jax.ShapeDtypeStruct((toks, d_model), BF16),
                   jax.ShapeDtypeStruct((experts, toks), F32)],
        scratch_shapes=[pltpu.VMEM((toks, w_out.shape[0]), BF16), pltpu.VMEM((8, d_model), F32),
                        pltpu.VMEM((depth, w_out.shape[0], tile), BF16), pltpu.SemaphoreType.DMA((1, depth))],
        compiler_params=pltpu.CompilerParams(dimension_semantics=("arbitrary",), vmem_limit_bytes=VMEM_CAP),
        cost_estimate=pl.CostEstimate(flops=2 * toks * d_model * d_model, bytes_accessed=2 * d_model * d_model, transcendentals=0),
        name="out_project",
    )(tokens, attn, w_out, *vec_rows, w_router_t, *routes)


def peer(me, flip):
    for bit in (1, 2, 4):
        if flip & bit:
            me = me + bit - 2 * bit * lax.rem(me // bit, 2)
    return me


PIECE = {(0, 0): 0, (0, 1): 1, (1, 0): 2, (1, 1): 3,
         (2, 0): 4, (4, 1): 5, (3, 0): 6, (5, 1): 7,
         (2, 1): 8, (4, 0): 9, (3, 1): 10, (5, 0): 11,
         (6, 0): 12, (6, 1): 13, (7, 0): 14, (7, 1): 15}


def moe_kernel(h_ref, gate_ref, x_ref, wg_hbm, wu_hbm, wd_hbm, out_ref,
               wg, wu, wd, hbuf, gates, wcol, zt_scr, z_scr, mine, first, dsend, drecv, yrecv, local_sem, send_sem, recv_sem):
    me = lax.axis_index('ep')
    toks, d_model = h_ref.shape
    ff = wg.shape[0]
    part = toks // 2
    parts = 4

    own = pltpu.make_async_copy(h_ref, hbuf.at[pl.ds(0, toks)], local_sem.at[0])
    own.start()
    loads = []
    for hbm, scr in ((wg_hbm, wg), (wu_hbm, wu), (wd_hbm, wd)):
        size = ff // 2
        for piece in range(2):
            rows = pl.ds(piece * size, size)
            loads.append(pltpu.make_async_copy(hbm.at[rows], scr.at[rows], local_sem.at[1 + len(loads)]))

    barrier = pltpu.get_barrier_semaphore()
    for flip in range(1, 8):
        pl.semaphore_signal(barrier, inc=1, device_id=(peer(me, flip),), device_id_type=pl.DeviceIdType.MESH)
    pl.semaphore_wait(barrier, 7)

    def remote(num, src, dst, flip):
        return pltpu.make_async_remote_copy(src_ref=src, dst_ref=dst, send_sem=send_sem.at[num], recv_sem=recv_sem.at[num],
                                            device_id=(peer(me, flip),), device_id_type=pl.DeviceIdType.MESH)

    def piece(flip, half):
        return hbuf.at[pl.ds(PIECE[(flip, half)] * part, part)]

    def pass_on(num, source, half, flip):
        return remote(num, piece(source, half), piece(source ^ flip, half), flip)

    sends = {}
    for num, half, flip in ((0, 0, 2), (3, 1, 4), (1, 1, 2), (2, 0, 4)):
        sends[num] = pass_on(num, 0, half, flip)
    sends[4] = remote(4, hbuf.at[pl.ds(0, toks)], hbuf.at[pl.ds(toks, toks)], 1)
    for num, source, half, flip in ((5, 2, 0, 4), (6, 4, 1, 2), (7, 2, 0, 1), (8, 2, 1, 1), (9, 4, 0, 1), (10, 4, 1, 1), (11, 6, 0, 1), (12, 6, 1, 1)):
        sends[num] = pass_on(num, source, half, flip)
    for flip in range(1, 8):
        sends[12 + flip] = remote(12 + flip, gate_ref, gates.at[flip], flip)
    order = (0, 3, 1, 2)
    for turn, blk in enumerate(order):
        sends[20 + blk] = remote(20 + blk, dsend.at[turn % 2], drecv.at[blk], 1)
    lower, upper = pl.ds(0, part), pl.ds(part, part)
    sends[24] = remote(24, drecv.at[1, lower], yrecv.at[0, lower], 2)
    sends[25] = remote(25, drecv.at[1, upper], yrecv.at[1, upper], 4)
    sends[26] = remote(26, drecv.at[2, lower], yrecv.at[0, upper], 2)
    sends[27] = remote(27, drecv.at[2, upper], yrecv.at[1, lower], 4)
    sends[28] = remote(28, drecv.at[3, lower], yrecv.at[2, upper], 2)
    sends[29] = remote(29, drecv.at[3, upper], yrecv.at[2, lower], 4)

    own.wait()
    for num in (0, 3, 4):
        sends[num].start()
    for flip in range(1, 8):
        sends[12 + flip].start()
    for load in loads:
        load.start()
    gates[0] = gate_ref[...]
    for flip in range(1, 8):
        sends[12 + flip].wait_recv()
    same = lax.broadcasted_iota(jnp.int32, (toks, toks), 0) == lax.broadcasted_iota(jnp.int32, (toks, toks), 1)
    for flip in range(8):
        col = jnp.sum(jnp.where(same, gates[flip, pl.ds(me, 1), :], 0.0), axis=1, keepdims=True)
        for half in range(2):
            wcol[pl.ds(PIECE[(flip, half)] * part, part), :] = col[half * part:(half + 1) * part]

    def hidden(blk):
        size = ff // 2

        @pl.loop(0, 2)
        def _(idx):
            rows = pl.ds(pl.multiple_of(idx * size, 16), size)
            h_blk = hbuf[pl.ds(blk * 2 * toks, 2 * toks), :]
            nt = (((1,), (1,)), ((), ()))
            u_val = lax.dot_general(wg[rows, :], h_blk, nt, preferred_element_type=F32)
            v_val = lax.dot_general(wu[rows, :], h_blk, nt, preferred_element_type=F32)
            zt_scr[rows, :] = jax.nn.silu(u_val) * v_val

        z_scr[...] = zt_scr[...].T.astype(BF16)

    tile = 512

    def down(blk, first_row, store):
        rows = pl.ds(blk * 2 * toks + first_row, toks)

        @pl.loop(0, d_model // tile)
        def _(idx):
            cols = pl.ds(pl.multiple_of(idx * tile, tile), tile)
            val = jnp.dot(z_scr[pl.ds(first_row, toks), :], wd[:, cols], preferred_element_type=F32).astype(BF16)
            store(cols, wcol[rows, :] * val.astype(F32))

    def keep_theirs(turn):
        def store(cols, val):
            dsend[turn % 2, :, cols] = val.astype(BF16)
        return store

    def keep_mine(cols, val):
        mine[:, cols] = val

    def merge(blk):
        @pl.loop(0, d_model // tile)
        def _(idx):
            cols = pl.ds(pl.multiple_of(idx * tile, tile), tile)
            total = mine[:, cols] + drecv[blk, :, cols].astype(F32)
            if blk == 2:
                total = total + yrecv[2, :, cols].astype(F32)
            if blk == 0:
                first[:, cols] = total
            else:
                drecv[blk, :, cols] = total.astype(BF16)

    def forward(arrived, nums):
        for num in arrived:
            sends[num].wait_recv()
        for num in nums:
            sends[num].start()

    forward((0, 3), (5, 6, 7, 10, 1, 2))
    for load in loads:
        load.wait()
    sends[4].wait_recv()
    homeward = {0: (), 3: (28, 29), 1: (24, 25), 2: (26, 27)}
    needs = {0: (), 3: (11, 12), 1: (7, 10), 2: (8, 9)}
    for turn, blk in enumerate(order):
        for num in needs[blk]:
            sends[num].wait_recv()
        hidden(blk)
        if turn >= 2:
            sends[20 + order[turn - 2]].wait_send()
        down(blk, toks, keep_theirs(turn))
        sends[20 + blk].start()
        down(blk, 0, keep_mine)
        if blk == 0:
            forward((5, 6), (11, 12))
        sends[20 + blk].wait_recv()
        if blk == 2:
            for num in (28, 29):
                sends[num].wait_recv()
        merge(blk)
        for num in homeward[blk]:
            sends[num].start()
        if blk == 3:
            forward((1, 2), (8, 9))

    for num in range(24, 28):
        sends[num].wait_recv()

    @pl.loop(0, d_model // tile)
    def _(idx):
        cols = pl.ds(pl.multiple_of(idx * tile, tile), tile)
        total = first[:, cols] + yrecv[0, :, cols].astype(F32) + yrecv[1, :, cols].astype(F32)
        out_ref[:, cols] = (x_ref[:, cols].astype(F32) + total).astype(BF16)

    for num in list(range(20)) + [21, 22] + list(range(24, 30)):
        sends[num].wait_send()


def expert_exchange(h_two, gates, x_mid, w_gate_t, w_up_t, w_down):
    toks, d_model = h_two.shape
    ff = w_down.shape[0]
    experts = gates.shape[0]
    hbm = pl.BlockSpec(memory_space=pl.ANY)
    vmem = pl.BlockSpec(memory_space=pltpu.VMEM)
    return pl.pallas_call(
        moe_kernel,
        in_specs=[hbm, vmem, vmem, hbm, hbm, hbm],
        out_specs=vmem,
        out_shape=jax.ShapeDtypeStruct((toks, d_model), BF16),
        scratch_shapes=[
            pltpu.VMEM((ff, d_model), BF16), pltpu.VMEM((ff, d_model), BF16), pltpu.VMEM((ff, d_model), BF16),
            pltpu.VMEM((8 * toks, d_model), BF16),
            pltpu.VMEM((8, experts, toks), F32),
            pltpu.VMEM((8 * toks, 1), F32),
            pltpu.VMEM((ff, 2 * toks), F32),
            pltpu.VMEM((2 * toks, ff), BF16),
            pltpu.VMEM((toks, d_model), F32),
            pltpu.VMEM((toks, d_model), F32),
            pltpu.VMEM((2, toks, d_model), BF16),
            pltpu.VMEM((4, toks, d_model), BF16),
            pltpu.VMEM((3, toks, d_model), BF16),
            pltpu.SemaphoreType.DMA((7,)),
            pltpu.SemaphoreType.DMA((30,)),
            pltpu.SemaphoreType.DMA((30,)),
        ],
        compiler_params=pltpu.CompilerParams(collective_id=0, has_side_effects=True, vmem_limit_bytes=67043328),
        cost_estimate=pl.CostEstimate(flops=48 * toks * d_model * ff, bytes_accessed=6 * d_model * ff, transcendentals=0),
        name="expert_exchange",
    )(h_two, gates, x_mid, w_gate_t, w_up_t, w_down)


def solution(mesh):
    def local_step(tokens, k_cache, v_cache, positions, expert_one, expert_two, eligible, ln1_gain, ln1_bias, w_query, b_query, w_key, b_key, w_value, b_value, w_out, b_out, ln2_gain, ln2_bias, w_router, w_gate, w_up, w_down):
        toks, seq, heads, hd = k_cache.shape
        cos_tab, sin_tab = rope_tables(positions, hd)
        lanes = lambda vec: vec.reshape(-1, 128)
        routes = (expert_one.reshape(1, toks), expert_two.reshape(1, toks), eligible.T)
        q_rot, key_new, value_new = (v.reshape(toks, heads, hd) for v in qkv_project(tokens, tuple(map(lanes, (ln1_gain, ln1_bias, b_query, b_key, b_value))), cos_tab, sin_tab, w_query, w_key, w_value))
        attn = attend(positions, q_rot, key_new, value_new, k_cache, v_cache)
        x_mid, h_two, gates = out_project(tokens, attn.reshape(toks * heads, hd), w_out, tuple(map(lanes, (b_out, ln2_gain, ln2_bias))), w_router.T, routes)
        tokens_out = expert_exchange(h_two, gates, x_mid, w_gate[0].T, w_up[0].T, w_down[0])
        return tokens_out, key_new, value_new

    row_spec = P('ep', None)
    cache_spec = P('ep', None, None, None)
    vec_spec = P('ep')
    rep_one = P(None)
    rep_two = P(None, None)
    expert_spec = P('ep', None, None)
    in_specs = (row_spec, cache_spec, cache_spec, vec_spec, vec_spec, vec_spec, row_spec, rep_one, rep_one, rep_two, rep_one, rep_two, rep_one, rep_two, rep_one, rep_two, rep_one, rep_one, rep_one, rep_two, expert_spec, expert_spec, expert_spec)
    out_specs = (row_spec, expert_spec, expert_spec)
    return jax.shard_map(local_step, mesh=mesh, in_specs=in_specs, out_specs=out_specs, check_vma=False)
```

```python
import functools

import jax
import jax.numpy as jnp
from jax import lax
from jax.experimental import pallas as pl
from jax.experimental.pallas import tpu as pltpu
from jax.sharding import PartitionSpec as P

ROPE_BASE = 10000.0
LN_EPS = 1e-5
VMEM_CAP = 60 * 1024 * 1024
F32 = jnp.float32
BF16 = jnp.bfloat16


def layer_norm(values_in, gain, bias):
    mean_val = jnp.mean(values_in, axis=-1, keepdims=True)
    centered = values_in - mean_val
    var_val = jnp.mean(centered * centered, axis=-1, keepdims=True)
    return centered * lax.rsqrt(var_val + LN_EPS) * gain.astype(F32) + bias.astype(F32)


def rope_tables(positions, head_dim):
    half_dim = head_dim // 2
    inv_freq = ROPE_BASE ** (jnp.arange(half_dim, dtype=F32) * (-2.0 / head_dim))
    angles = positions.astype(F32)[:, None] * inv_freq[None, :]
    cos_half, sin_half = jnp.cos(angles), jnp.sin(angles)
    return jnp.concatenate([cos_half, cos_half], axis=-1), jnp.concatenate([-sin_half, sin_half], axis=-1)


def ring(step, steps, depth, copies):
    @pl.when(step == 0)
    def _():
        for idx in range(depth - 1):
            for copy in copies(idx):
                copy.start()

    @pl.when(step + depth - 1 < steps)
    def _():
        for copy in copies(step + depth - 1):
            copy.start()

    for copy in copies(step):
        copy.wait()


def column_copies(hbms, bufs, sems, tile, depth):
    def copies(idx):
        slot = lax.rem(idx, depth) if not isinstance(idx, int) else idx % depth
        start = pl.multiple_of(idx * tile, tile) if not isinstance(idx, int) else idx * tile
        return [pltpu.make_async_copy(hbm.at[:, pl.ds(start, tile)], buf.at[slot], sems.at[num, slot])
                for num, (hbm, buf) in enumerate(zip(hbms, bufs))]
    return copies


def as_row(dst, row, vec_ref):
    width = vec_ref.shape[1]
    vals = vec_ref[...].astype(F32)
    for idx in range(vec_ref.shape[0]):
        dst[row:row + 1, idx * width:(idx + 1) * width] = vals[idx:idx + 1, :]


def qkv_kernel(heads, x_ref, g_ref, b_ref, bq_ref, bk_ref, bv_ref, cos_ref, sin_ref, wq_hbm, wk_hbm, wv_hbm, q_out, k_out, v_out,
               h_scr, q_scr, k_scr, v_scr, vec_ref, wq_buf, wk_buf, wv_buf, sems):
    step = pl.program_id(0)
    toks = x_ref.shape[0]
    hd = cos_ref.shape[1]
    depth, _, tile = wq_buf.shape
    slot = lax.rem(step, depth)
    ring(step, pl.num_programs(0), depth, column_copies((wq_hbm, wk_hbm, wv_hbm), (wq_buf, wk_buf, wv_buf), sems, tile, depth))

    @pl.when(step == 0)
    def _():
        for row, ref in enumerate((g_ref, b_ref, bq_ref, bk_ref, bv_ref)):
            as_row(vec_ref, row, ref)
        h_scr[...] = layer_norm(x_ref[...].astype(F32), vec_ref[0:1, :], vec_ref[1:2, :]).astype(BF16)

    h_one = h_scr[...]
    cols = pl.ds(pl.multiple_of(step * tile, tile), tile)
    per_step = tile // hd
    for row, w_buf, scr in ((2, wq_buf, q_scr), (3, wk_buf, k_scr), (4, wv_buf, v_scr)):
        lin = jnp.dot(h_one, w_buf[slot], preferred_element_type=F32) + vec_ref[row:row + 1, cols]
        for sub in range(per_step):
            part = lin[:, sub * hd:(sub + 1) * hd]
            if row < 4:
                part = part * cos_ref[...] + pltpu.roll(part, hd // 2, 1) * sin_ref[...]
            scr[pl.ds(step * per_step + sub, toks, stride=heads), :] = part

    @pl.when(step == pl.num_programs(0) - 1)
    def _():
        for scr, out in ((q_scr, q_out), (k_scr, k_out), (v_scr, v_out)):
            out[...] = scr[...].astype(BF16)


def full_spec(shape):
    return pl.BlockSpec(shape, lambda *ids: (0,) * len(shape))


def qkv_project(tokens, rows, cos_tab, sin_tab, wq, wk, wv):
    toks, d_model = tokens.shape
    hd = cos_tab.shape[1]
    heads = wq.shape[1] // hd
    tile, depth = 256, 4
    w_spec = pl.BlockSpec(memory_space=pl.ANY)
    out = jax.ShapeDtypeStruct((toks * heads, hd), BF16)
    return pl.pallas_call(
        functools.partial(qkv_kernel, heads),
        grid=(wq.shape[1] // tile,),
        in_specs=[full_spec((toks, d_model))] + [full_spec(row.shape) for row in rows] + [full_spec((toks, hd)), full_spec((toks, hd)), w_spec, w_spec, w_spec],
        out_specs=[full_spec((toks * heads, hd))] * 3,
        out_shape=[out] * 3,
        scratch_shapes=[pltpu.VMEM((toks, d_model), BF16)] + [pltpu.VMEM((toks * heads, hd), F32)] * 3
        + [pltpu.VMEM((8, d_model), F32)] + [pltpu.VMEM((depth, d_model, tile), BF16)] * 3 + [pltpu.SemaphoreType.DMA((3, depth))],
        compiler_params=pltpu.CompilerParams(dimension_semantics=("arbitrary",), vmem_limit_bytes=VMEM_CAP),
        cost_estimate=pl.CostEstimate(flops=6 * toks * d_model * wq.shape[1], bytes_accessed=6 * d_model * wq.shape[1], transcendentals=0),
        name="qkv_project",
    )(tokens, *rows, cos_tab, sin_tab, wq, wk, wv)


def attend_kernel(pos_ref, q_ref, kn_ref, vn_ref, k_hbm, v_hbm, o_ref, k_buf, v_buf, sems):
    depth, blk, seq, heads, hd = k_buf.shape
    step = pl.program_id(0)

    def copies(idx):
        slot = lax.rem(idx, depth) if not isinstance(idx, int) else idx % depth
        return [pltpu.make_async_copy(hbm.at[pl.ds(idx * blk, blk)], buf.at[slot], sems.at[num, slot])
                for num, (hbm, buf) in enumerate(((k_hbm, k_buf), (v_hbm, v_buf)))]

    ring(step, pl.num_programs(0), depth, copies)
    k_ref, v_ref = k_buf.at[lax.rem(step, depth)], v_buf.at[lax.rem(step, depth)]
    groups = 128 // heads
    scale = hd ** -0.5
    rows = seq // groups
    half = rows // 2
    two = 2 * heads
    r_id = lax.broadcasted_iota(jnp.int32, (two, 128), 0)
    l_id = lax.broadcasted_iota(jnp.int32, (two, 128), 1)
    pick = (l_id // two == r_id // heads) & (l_id % heads == r_id % heads)
    diag = lax.broadcasted_iota(jnp.int32, (heads, 128), 1) % heads == lax.broadcasted_iota(jnp.int32, (heads, 128), 0)
    s_id = groups * lax.broadcasted_iota(jnp.int32, (rows, 128), 0) + lax.broadcasted_iota(jnp.int32, (rows, 128), 1) // heads
    zero_q = jnp.zeros((heads, hd), BF16)

    def all_groups(vals, op):
        vals = op(vals, pltpu.roll(vals, heads, 1))
        return op(vals, pltpu.roll(vals, 2 * heads, 1))

    s_list = []
    for tok in range(blk):
        pos = pos_ref[pl.program_id(0) * blk + tok]
        q_tok = q_ref[tok]
        top = jnp.concatenate([q_tok, zero_q], axis=1)
        bot = jnp.concatenate([zero_q, q_tok], axis=1)
        q_mat = jnp.concatenate([top, bot, top, bot], axis=0)
        k_tok = k_ref[tok].reshape(seq // 2, 2, heads, hd)
        k_mat = jnp.concatenate([k_tok[:, 0].reshape(seq // 2 * heads, hd), k_tok[:, 1].reshape(seq // 2 * heads, hd)], axis=1)
        raw = lax.dot_general(k_mat, q_mat, (((1,), (1,)), ((), ())), preferred_element_type=F32)
        s_tok = jnp.sum(jnp.where(pick[None], raw.reshape(rows, two, 128), 0.0), axis=1) * scale
        s_list.append(jnp.where(s_id < pos, s_tok, -jnp.inf)[None])
    s_cache = jnp.concatenate(s_list, axis=0)
    new_col = jnp.sum(q_ref[...].astype(F32) * kn_ref[...].astype(F32), axis=2, keepdims=True)
    s_new = jnp.sum(jnp.where(diag[None], new_col, 0.0), axis=1) * scale
    top_val = jnp.maximum(all_groups(jnp.max(s_cache, axis=1), jnp.maximum), s_new)
    e_cache = jnp.exp(s_cache - top_val[:, None, :])
    e_new = jnp.exp(s_new - top_val)
    denom = all_groups(jnp.sum(e_cache, axis=1), jnp.add) + e_new
    p_cache = e_cache / denom[:, None, :]
    p_new = (e_new / denom).astype(BF16).astype(F32)
    lane_id = lax.broadcasted_iota(jnp.int32, (heads, 128), 1)
    once = diag & (lane_id < heads)
    p_col = jnp.sum(jnp.where(once[None], p_new[:, None, :], 0.0), axis=2, keepdims=True)
    for tok in range(blk):
        p_rows = [jnp.where(diag, p_cache[tok, r:r + 1, :], 0.0).astype(BF16) for r in range(rows)]
        p_mat = jnp.concatenate([jnp.concatenate(p_rows[:half], axis=1), jnp.concatenate(p_rows[half:], axis=1)], axis=0)
        v_tok = v_ref[tok].reshape(2, seq // 2 * heads, hd)
        v_mat = jnp.concatenate([v_tok[0], v_tok[1]], axis=1)
        vals = jnp.dot(p_mat, v_mat, preferred_element_type=F32)
        o_ref[tok] = vals[:heads, :hd] + vals[heads:, hd:] + p_col[tok] * vn_ref[tok].astype(F32)


def attend(positions, q_rot, key_new, value_new, k_cache, v_cache):
    toks, seq, heads, hd = k_cache.shape
    blk, depth = 4, 5
    row = pl.BlockSpec((blk, heads, hd), lambda i, pos: (i, 0, 0))
    cache = pl.BlockSpec(memory_space=pl.ANY)
    ring_buf = pltpu.VMEM((depth, blk, seq, heads, hd), BF16)
    return pl.pallas_call(
        attend_kernel,
        grid_spec=pltpu.PrefetchScalarGridSpec(
            num_scalar_prefetch=1, grid=(toks // blk,),
            in_specs=[row, row, row, cache, cache], out_specs=row,
            scratch_shapes=[ring_buf, ring_buf, pltpu.SemaphoreType.DMA((2, depth))]),
        out_shape=jax.ShapeDtypeStruct((toks, heads, hd), F32),
        compiler_params=pltpu.CompilerParams(dimension_semantics=("arbitrary",), vmem_limit_bytes=VMEM_CAP),
        cost_estimate=pl.CostEstimate(flops=4 * toks * seq * heads * hd * 32, bytes_accessed=4 * toks * seq * heads * hd, transcendentals=0),
        name="attend",
    )(positions, q_rot, key_new, value_new, k_cache, v_cache)


def out_kernel(heads, x_ref, a_ref, w_hbm, bo_ref, g_ref, b_ref, wr_ref, e1_ref, e2_ref, el_ref, x1_out, h2_out, g_out, a_scr, vec_ref, w_buf, sems):
    step = pl.program_id(0)
    toks = x_ref.shape[0]
    hd = a_ref.shape[1]
    depth, _, tile = w_buf.shape
    experts = wr_ref.shape[0]
    ring(step, pl.num_programs(0), depth, column_copies((w_hbm,), (w_buf,), sems, tile, depth))

    @pl.when(step == 0)
    def _():
        for row, ref in enumerate((bo_ref, g_ref, b_ref)):
            as_row(vec_ref, row, ref)
        for head in range(heads):
            a_scr[:, head * hd:(head + 1) * hd] = a_ref[pl.ds(head, toks, stride=heads), :].astype(BF16)

    cols = pl.ds(pl.multiple_of(step * tile, tile), tile)
    lin = jnp.dot(a_scr[...], w_buf[lax.rem(step, depth)], preferred_element_type=F32)
    x1_out[:, cols] = (x_ref[:, cols].astype(F32) + lin + vec_ref[0:1, cols]).astype(BF16)

    @pl.when(step == pl.num_programs(0) - 1)
    def _():
        h_two = layer_norm(x1_out[...].astype(F32), vec_ref[1:2, :], vec_ref[2:3, :]).astype(BF16)
        h2_out[...] = h_two
        logits = lax.dot_general(wr_ref[...], h_two, (((1,), (1,)), ((), ())), preferred_element_type=F32)
        ids = lax.broadcasted_iota(jnp.int32, logits.shape, 0)
        hit_one, hit_two = ids == e1_ref[...], ids == e2_ref[...]
        keep_one = el_ref[...] == 1
        keep_two = keep_one & jnp.logical_not(hit_one)

        def prob(keep):
            masked = jnp.where(keep, logits, -jnp.inf)
            expd = jnp.exp(masked - jnp.max(masked, axis=0, keepdims=True))
            return expd / jnp.sum(expd, axis=0, keepdims=True)

        g_out[...] = jnp.where(hit_one, prob(keep_one), 0.0) + jnp.where(hit_two, prob(keep_two), 0.0)


def out_project(tokens, attn, w_out, vec_rows, w_router_t, routes):
    toks, d_model = tokens.shape
    rows, hd = attn.shape
    tile, depth = 256, 6
    experts = w_router_t.shape[0]
    return pl.pallas_call(
        functools.partial(out_kernel, rows // toks),
        grid=(d_model // tile,),
        in_specs=[full_spec((toks, d_model)), full_spec((rows, hd)), pl.BlockSpec(memory_space=pl.ANY)]
        + [full_spec(row.shape) for row in vec_rows] + [full_spec((experts, d_model))] + [full_spec(route.shape) for route in routes],
        out_specs=[full_spec((toks, d_model)), full_spec((toks, d_model)), full_spec((experts, toks))],
        out_shape=[jax.ShapeDtypeStruct((toks, d_model), BF16), jax.ShapeDtypeStruct((toks, d_model), BF16),
                   jax.ShapeDtypeStruct((experts, toks), F32)],
        scratch_shapes=[pltpu.VMEM((toks, w_out.shape[0]), BF16), pltpu.VMEM((8, d_model), F32),
                        pltpu.VMEM((depth, w_out.shape[0], tile), BF16), pltpu.SemaphoreType.DMA((1, depth))],
        compiler_params=pltpu.CompilerParams(dimension_semantics=("arbitrary",), vmem_limit_bytes=VMEM_CAP),
        cost_estimate=pl.CostEstimate(flops=2 * toks * d_model * d_model, bytes_accessed=2 * d_model * d_model, transcendentals=0),
        name="out_project",
    )(tokens, attn, w_out, *vec_rows, w_router_t, *routes)


def peer(me, flip):
    for bit in (1, 2, 4):
        if flip & bit:
            me = me + bit - 2 * bit * lax.rem(me // bit, 2)
    return me


PIECE = {(0, 0): 0, (0, 1): 1, (1, 0): 2, (1, 1): 3,
         (2, 0): 4, (4, 1): 5, (3, 0): 6, (5, 1): 7,
         (2, 1): 8, (4, 0): 9, (3, 1): 10, (5, 0): 11,
         (6, 0): 12, (6, 1): 13, (7, 0): 14, (7, 1): 15}


def moe_kernel(h_ref, gate_ref, x_ref, wg_hbm, wu_hbm, wd_hbm, out_ref,
               wg, wu, wd, hbuf, gates, wcol, zt_scr, z_scr, mine, first, dsend, drecv, yrecv, local_sem, send_sem, recv_sem):
    me = lax.axis_index('ep')
    toks, d_model = h_ref.shape
    ff = wg.shape[0]
    part = toks // 2
    parts = 4

    own = pltpu.make_async_copy(h_ref, hbuf.at[pl.ds(0, toks)], local_sem.at[0])
    own.start()
    loads = []
    for hbm, scr in ((wg_hbm, wg), (wu_hbm, wu), (wd_hbm, wd)):
        size = ff // 2
        for piece in range(2):
            rows = pl.ds(piece * size, size)
            loads.append(pltpu.make_async_copy(hbm.at[rows], scr.at[rows], local_sem.at[1 + len(loads)]))

    barrier = pltpu.get_barrier_semaphore()
    for flip in range(1, 8):
        pl.semaphore_signal(barrier, inc=1, device_id=(peer(me, flip),), device_id_type=pl.DeviceIdType.MESH)
    pl.semaphore_wait(barrier, 7)

    def remote(num, src, dst, flip):
        return pltpu.make_async_remote_copy(src_ref=src, dst_ref=dst, send_sem=send_sem.at[num], recv_sem=recv_sem.at[num],
                                            device_id=(peer(me, flip),), device_id_type=pl.DeviceIdType.MESH)

    def piece(flip, half):
        return hbuf.at[pl.ds(PIECE[(flip, half)] * part, part)]

    def pass_on(num, source, half, flip):
        return remote(num, piece(source, half), piece(source ^ flip, half), flip)

    sends = {}
    for num, half, flip in ((0, 0, 2), (3, 1, 4), (1, 1, 2), (2, 0, 4)):
        sends[num] = pass_on(num, 0, half, flip)
    sends[4] = remote(4, hbuf.at[pl.ds(0, toks)], hbuf.at[pl.ds(toks, toks)], 1)
    for num, source, half, flip in ((5, 2, 0, 4), (6, 4, 1, 2), (7, 2, 0, 1), (8, 2, 1, 1), (9, 4, 0, 1), (10, 4, 1, 1), (11, 6, 0, 1), (12, 6, 1, 1)):
        sends[num] = pass_on(num, source, half, flip)
    for flip in range(1, 8):
        sends[12 + flip] = remote(12 + flip, gate_ref, gates.at[flip], flip)
    order = (0, 3, 1, 2)
    for turn, blk in enumerate(order):
        sends[20 + blk] = remote(20 + blk, dsend.at[turn % 2], drecv.at[blk], 1)
    lower, upper = pl.ds(0, part), pl.ds(part, part)
    sends[24] = remote(24, drecv.at[1, lower], yrecv.at[0, lower], 2)
    sends[25] = remote(25, drecv.at[1, upper], yrecv.at[1, upper], 4)
    sends[26] = remote(26, drecv.at[2, lower], yrecv.at[0, upper], 2)
    sends[27] = remote(27, drecv.at[2, upper], yrecv.at[1, lower], 4)
    sends[28] = remote(28, drecv.at[3, lower], yrecv.at[2, upper], 2)
    sends[29] = remote(29, drecv.at[3, upper], yrecv.at[2, lower], 4)

    own.wait()
    for num in (0, 3, 4):
        sends[num].start()
    for flip in range(1, 8):
        sends[12 + flip].start()
    early = (loads[0], loads[2])
    late = (loads[1], loads[3], loads[4], loads[5])
    for load in early:
        load.start()
    gates[0] = gate_ref[...]
    for flip in range(1, 8):
        sends[12 + flip].wait_recv()
    same = lax.broadcasted_iota(jnp.int32, (toks, toks), 0) == lax.broadcasted_iota(jnp.int32, (toks, toks), 1)
    for flip in range(8):
        col = jnp.sum(jnp.where(same, gates[flip, pl.ds(me, 1), :], 0.0), axis=1, keepdims=True)
        for half in range(2):
            wcol[pl.ds(PIECE[(flip, half)] * part, part), :] = col[half * part:(half + 1) * part]

    def hidden(blk, first_trip=0, last_trip=2):
        size = ff // 2

        @pl.loop(first_trip, last_trip)
        def _(idx):
            rows = pl.ds(pl.multiple_of(idx * size, 16), size)
            h_blk = hbuf[pl.ds(blk * 2 * toks, 2 * toks), :]
            nt = (((1,), (1,)), ((), ()))
            u_val = lax.dot_general(wg[rows, :], h_blk, nt, preferred_element_type=F32)
            v_val = lax.dot_general(wu[rows, :], h_blk, nt, preferred_element_type=F32)
            zt_scr[rows, :] = jax.nn.silu(u_val) * v_val

        if last_trip == 2:
            z_scr[...] = zt_scr[...].T.astype(BF16)

    tile = 512

    def down(blk, first_row, store):
        rows = pl.ds(blk * 2 * toks + first_row, toks)

        @pl.loop(0, d_model // tile)
        def _(idx):
            cols = pl.ds(pl.multiple_of(idx * tile, tile), tile)
            val = jnp.dot(z_scr[pl.ds(first_row, toks), :], wd[:, cols], preferred_element_type=F32).astype(BF16)
            store(cols, wcol[rows, :] * val.astype(F32))

    def keep_theirs(turn):
        def store(cols, val):
            dsend[turn % 2, :, cols] = val.astype(BF16)
        return store

    def keep_mine(cols, val):
        mine[:, cols] = val

    def merge(blk):
        @pl.loop(0, d_model // tile)
        def _(idx):
            cols = pl.ds(pl.multiple_of(idx * tile, tile), tile)
            total = mine[:, cols] + drecv[blk, :, cols].astype(F32)
            if blk == 2:
                total = total + yrecv[2, :, cols].astype(F32)
            if blk == 0:
                first[:, cols] = total
            else:
                drecv[blk, :, cols] = total.astype(BF16)

    def forward(arrived, nums):
        for num in arrived:
            sends[num].wait_recv()
        for num in nums:
            sends[num].start()

    for load in early:
        load.wait()
    for load in late:
        load.start()
    sends[4].wait_recv()
    hidden(0, 0, 1)
    forward((0, 3), (5, 6, 7, 10, 1, 2))
    for load in late:
        load.wait()
    homeward = {0: (), 3: (28, 29), 1: (24, 25), 2: (26, 27)}
    needs = {0: (), 3: (11, 12), 1: (7, 10), 2: (8, 9)}
    for turn, blk in enumerate(order):
        for num in needs[blk]:
            sends[num].wait_recv()
        hidden(blk, 1 if blk == 0 else 0)
        if turn >= 2:
            sends[20 + order[turn - 2]].wait_send()
        down(blk, toks, keep_theirs(turn))
        sends[20 + blk].start()
        down(blk, 0, keep_mine)
        if blk == 0:
            forward((5, 6), (11, 12))
        sends[20 + blk].wait_recv()
        if blk == 2:
            for num in (28, 29):
                sends[num].wait_recv()
        merge(blk)
        for num in homeward[blk]:
            sends[num].start()
        if blk == 3:
            forward((1, 2), (8, 9))

    for num in range(24, 28):
        sends[num].wait_recv()

    @pl.loop(0, d_model // tile)
    def _(idx):
        cols = pl.ds(pl.multiple_of(idx * tile, tile), tile)
        total = first[:, cols] + yrecv[0, :, cols].astype(F32) + yrecv[1, :, cols].astype(F32)
        out_ref[:, cols] = (x_ref[:, cols].astype(F32) + total).astype(BF16)

    for num in list(range(20)) + [21, 22] + list(range(24, 30)):
        sends[num].wait_send()


def expert_exchange(h_two, gates, x_mid, w_gate_t, w_up_t, w_down):
    toks, d_model = h_two.shape
    ff = w_down.shape[0]
    experts = gates.shape[0]
    hbm = pl.BlockSpec(memory_space=pl.ANY)
    vmem = pl.BlockSpec(memory_space=pltpu.VMEM)
    return pl.pallas_call(
        moe_kernel,
        in_specs=[hbm, vmem, vmem, hbm, hbm, hbm],
        out_specs=vmem,
        out_shape=jax.ShapeDtypeStruct((toks, d_model), BF16),
        scratch_shapes=[
            pltpu.VMEM((ff, d_model), BF16), pltpu.VMEM((ff, d_model), BF16), pltpu.VMEM((ff, d_model), BF16),
            pltpu.VMEM((8 * toks, d_model), BF16),
            pltpu.VMEM((8, experts, toks), F32),
            pltpu.VMEM((8 * toks, 1), F32),
            pltpu.VMEM((ff, 2 * toks), F32),
            pltpu.VMEM((2 * toks, ff), BF16),
            pltpu.VMEM((toks, d_model), F32),
            pltpu.VMEM((toks, d_model), F32),
            pltpu.VMEM((2, toks, d_model), BF16),
            pltpu.VMEM((4, toks, d_model), BF16),
            pltpu.VMEM((3, toks, d_model), BF16),
            pltpu.SemaphoreType.DMA((7,)),
            pltpu.SemaphoreType.DMA((30,)),
            pltpu.SemaphoreType.DMA((30,)),
        ],
        compiler_params=pltpu.CompilerParams(collective_id=0, has_side_effects=True, vmem_limit_bytes=67043328),
        cost_estimate=pl.CostEstimate(flops=48 * toks * d_model * ff, bytes_accessed=6 * d_model * ff, transcendentals=0),
        name="expert_exchange",
    )(h_two, gates, x_mid, w_gate_t, w_up_t, w_down)


def solution(mesh):
    def local_step(tokens, k_cache, v_cache, positions, expert_one, expert_two, eligible, ln1_gain, ln1_bias, w_query, b_query, w_key, b_key, w_value, b_value, w_out, b_out, ln2_gain, ln2_bias, w_router, w_gate, w_up, w_down):
        toks, seq, heads, hd = k_cache.shape
        cos_tab, sin_tab = rope_tables(positions, hd)
        lanes = lambda vec: vec.reshape(-1, 128)
        routes = (expert_one.reshape(1, toks), expert_two.reshape(1, toks), eligible.T)
        q_rot, key_new, value_new = (v.reshape(toks, heads, hd) for v in qkv_project(tokens, tuple(map(lanes, (ln1_gain, ln1_bias, b_query, b_key, b_value))), cos_tab, sin_tab, w_query, w_key, w_value))
        attn = attend(positions, q_rot, key_new, value_new, k_cache, v_cache)
        x_mid, h_two, gates = out_project(tokens, attn.reshape(toks * heads, hd), w_out, tuple(map(lanes, (b_out, ln2_gain, ln2_bias))), w_router.T, routes)
        tokens_out = expert_exchange(h_two, gates, x_mid, w_gate[0].T, w_up[0].T, w_down[0])
        return tokens_out, key_new, value_new

    row_spec = P('ep', None)
    cache_spec = P('ep', None, None, None)
    vec_spec = P('ep')
    rep_one = P(None)
    rep_two = P(None, None)
    expert_spec = P('ep', None, None)
    in_specs = (row_spec, cache_spec, cache_spec, vec_spec, vec_spec, vec_spec, row_spec, rep_one, rep_one, rep_two, rep_one, rep_two, rep_one, rep_two, rep_one, rep_two, rep_one, rep_one, rep_one, rep_two, expert_spec, expert_spec, expert_spec)
    out_specs = (row_spec, expert_spec, expert_spec)
    return jax.shard_map(local_step, mesh=mesh, in_specs=in_specs, out_specs=out_specs, check_vma=False)
```
